512 devices in a mesh: section: 64 (over z, x, core), head: 8 (over y).
Axes of the slice: x: 4, y: 8, z: 8, core: 2. Of those that a mesh axis runs over, the one named last changes fastest.
Arguments:
- slice_rows: bfloat16 [8192, 4096], P('section', 'head'), may hold values from -6 to 6
- w_query: bfloat16 [4096, 4096], P(None, 'head'), may hold values from -0.09375 to 0.09375
- w_key: bfloat16 [4096, 1024], P(None, 'head'), may hold values from -0.09375 to 0.09375
- w_value: bfloat16 [4096, 1024], P(None, 'head'), may hold values from -0.09375 to 0.09375
- prefix_keys: bfloat16 [32768, 1024], P('section', 'head'), may hold values from -140 to 140
- prefix_values: bfloat16 [32768, 1024], P('section', 'head'), may hold values from -6 to 6
- prefix_blocks: int32 [64], replicated, may hold values from 1 to 2, as said below
Outputs:
- attention: bfloat16 [8192, 4096], P('section', 'head')
The draws below stay inside these ranges and needn't reach their ends.
Inputs may be any that keep to these rules, and one draw needn't show every extreme that they name: `prefix_blocks`: every section holds at least one live block; in every draw some section holds 2 blocks.
All inputs are finite; a program needn't handle non-finite values.
Results may differ from the reference program's by a relative error of at most 0.012.
The reference program's roundings to bfloat16 on the way (of `queries`) count: a program that leaves them out, or rounds other values in their place, can miss the bound.
Values may be sent and summed in bfloat16 or wider, within the bound.
A program may use at most 64 MiB of HBM per device.

```python
import math
import jax
import jax.numpy as jnp
from jax import lax

D = 4096
QHEADS = 32
KVHEADS = 8
HEAD_DIM = 128
BLOCK = 256
REACH = 7
SLICE = 128
PBLK = 2
PMAX = 512
SECTIONS = 64
TOKENS = 8192


def draw_prefix_keys(key, part):
    first_key = jax.random.fold_in(jax.random.fold_in(key, 11), 0)
    width = KVHEADS * HEAD_DIM
    whole = jax.random.normal(first_key, (SECTIONS, PMAX, width), jnp.float32)
    return whole.reshape(SECTIONS * PMAX, width).astype(jnp.bfloat16)


def draw_prefix_blocks(key, part):
    first_key, second_key, third_key = jax.random.split(jax.random.fold_in(key, 23), 3)
    modest = jax.random.randint(first_key, (SECTIONS,), 1, PBLK // 2 + 1)
    loaded = jax.random.randint(second_key, (SECTIONS,), 0, 8) == 0
    chosen = jax.random.randint(third_key, (), 0, SECTIONS)
    loaded = loaded | (jnp.arange(SECTIONS) == chosen)
    return jnp.where(loaded, PBLK, modest).astype(jnp.int32)


def block_scale(stream_key, shape, cuts, smallest, high):
    gain, own = 1.0, jax.random.fold_in(stream_key, 6)
    for axis_at, shards_of in cuts:
        draws = jnp.exp(jax.random.uniform(jax.random.fold_in(own, axis_at), (shards_of,), jnp.float32, smallest / len(cuts), high / len(cuts)))
        gain = gain * jnp.repeat(draws, shape[axis_at] // shards_of).reshape([-1 if axis == axis_at else 1 for axis in range(len(shape))])
    return gain


def scatter_about(own_key, shape, scale, reach, shards=(), kind=jnp.bfloat16):
    array = scale * jax.random.normal(own_key, shape, jnp.float32)
    if shards:
        array = array * block_scale(own_key, shape, shards, -0.22, 0.18)
    return jnp.clip(array, -reach, reach).astype(kind)


def setup_inputs(seed: int = 0) -> dict:
    keys = jax.random.split(jax.random.key(seed), 8)
    return {
        "slice_rows": scatter_about(keys[0], (TOKENS, D), 1.0, 6.0, ((0, 64), (1, 8))),
        "w_query": scatter_about(keys[1], (D, QHEADS * HEAD_DIM), D ** -0.5, 0.09375, ((1, 8),)),
        "w_key": scatter_about(keys[2], (D, KVHEADS * HEAD_DIM), D ** -0.5, 0.09375, ((1, 8),)),
        "w_value": scatter_about(keys[3], (D, KVHEADS * HEAD_DIM), D ** -0.5, 0.09375, ((1, 8),)),
        "prefix_keys": draw_prefix_keys(jax.random.fold_in(keys[7], 71), 0),
        "prefix_values": scatter_about(keys[5], (SECTIONS * PMAX, KVHEADS * HEAD_DIM), 1.0, 6.0, ((0, 64), (1, 8))),
        "prefix_blocks": draw_prefix_blocks(jax.random.fold_in(keys[7], 71), 0),
    }


def segment(queries, key_rows, values, live_mask):
    factor = 1.0 / math.sqrt(queries.shape[-1])
    scores = jnp.einsum('thge,khe->hgtk', queries.astype(jnp.float32), key_rows.astype(jnp.float32)) * factor
    scores = jnp.where(live_mask, scores, -1e+30)
    row_max = lax.optimization_barrier(jnp.max(scores, axis=-1))
    weights = jnp.where(live_mask, jnp.exp(scores - row_max[..., None]), 0.0)
    totals = lax.optimization_barrier(jnp.sum(weights, axis=-1))
    rounded = weights.astype(jnp.bfloat16)
    result = jnp.einsum('hgtk,khe->thge', rounded.astype(jnp.float32), values.astype(jnp.float32))
    return (row_max, totals, result)

def spread_scale(factor):
    return jnp.moveaxis(factor, 2, 0)[..., None]

def combine(first_part, second_part):
    row_max = jnp.maximum(first_part[0], second_part[0])
    first_scale = jnp.exp(first_part[0] - row_max)
    second_scale = jnp.exp(second_part[0] - row_max)
    totals = first_part[1] * first_scale + second_part[1] * second_scale
    result = first_part[2] * spread_scale(first_scale) + second_part[2] * spread_scale(second_scale)
    return (row_max, totals, result)

def reference(slice_rows, w_query, w_key, w_value, prefix_keys, prefix_values, prefix_blocks):
    group_size = QHEADS // KVHEADS
    queries = jnp.dot(slice_rows, w_query, preferred_element_type=jnp.float32).astype(jnp.bfloat16)
    own_keys = jnp.dot(slice_rows, w_key, preferred_element_type=jnp.float32).astype(jnp.bfloat16)
    own_values = jnp.dot(slice_rows, w_value, preferred_element_type=jnp.float32).astype(jnp.bfloat16)
    positions = jnp.arange(PMAX).astype(jnp.int32)
    causal = jnp.arange(SLICE)[:, None] >= jnp.arange(SLICE)[None, :]
    sections_all = jnp.arange(SECTIONS).astype(jnp.int32)

    def per_section(section_index):
        first_row = (section_index * SLICE).astype(jnp.int32)
        local_q = lax.dynamic_slice_in_dim(queries, first_row, SLICE, 0).reshape(SLICE, KVHEADS, group_size, HEAD_DIM)
        local_k = lax.dynamic_slice_in_dim(own_keys, first_row, SLICE, 0).reshape(SLICE, KVHEADS, HEAD_DIM)
        local_v = lax.dynamic_slice_in_dim(own_values, first_row, SLICE, 0).reshape(SLICE, KVHEADS, HEAD_DIM)
        merged = segment(local_q, local_k, local_v, causal)
        for offset in range(REACH + 1):
            owner_section = (section_index - offset).astype(jnp.int32)
            blocks = jnp.sum(jnp.where(sections_all == owner_section, prefix_blocks, 0)).astype(jnp.int32)
            live_mask = (positions < blocks * BLOCK)[None, :]
            base_row = (jnp.maximum(owner_section, 0) * PMAX).astype(jnp.int32)
            held_k = lax.dynamic_slice_in_dim(prefix_keys, base_row, PMAX, 0).reshape(PMAX, KVHEADS, HEAD_DIM)
            held_v = lax.dynamic_slice_in_dim(prefix_values, base_row, PMAX, 0).reshape(PMAX, KVHEADS, HEAD_DIM)
            merged = combine(merged, segment(local_q, held_k, held_v, live_mask))
        final = merged[2] / spread_scale(merged[1])
        return final.reshape(SLICE, QHEADS * HEAD_DIM).astype(jnp.bfloat16)
    stacked = lax.map(per_section, sections_all)
    return stacked.reshape(SECTIONS * SLICE, QHEADS * HEAD_DIM)
```

```python
import functools
import math

import jax
import jax.numpy as jnp
from jax import lax
from jax.experimental import pallas as pl
from jax.experimental.pallas import tpu as pltpu
from jax.sharding import PartitionSpec as P

HEAD_DIM = 128
BLOCK = 256
REACH = 7
COLUMNS = 4
LAYERS = 8
RING = 8
HALF = 64
MESH = pl.DeviceIdType.MESH

DIRECT = [4.2, 5.6, 7.0, 8.4]
ALONE = [3.5, 4.2, 4.9, 5.6]
SECOND = [7.3, 8.7, 10.1, 11.5]
THIRD = [10.4, 11.8, 13.2, 14.6]
LOW_FIRST = [0, 1, 2, 3]
HIGH_FIRST = [2, 3, 0, 1]
LOW, HIGH = (0, 1), (2, 3)


def rows_of(piece):
    return pl.ds((piece // 2) * BLOCK, BLOCK)


def arrivals(column):
    events = []

    def add(times, slot, order, right=(), left=(), up=(), pass_on="both"):
        for time, piece in zip(times, order):
            events.append((time, slot, piece, piece in right, piece in left, piece in up, pass_on))

    every = LOW + HIGH
    if column == 0:
        add(ALONE, 0, LOW_FIRST, pass_on="own")
        add(DIRECT, "relay", LOW_FIRST, up=every, pass_on="none")
        add(SECOND, 1, LOW_FIRST)
        add(SECOND, 3, LOW_FIRST, right=LOW)
        add(THIRD, 2, LOW_FIRST)
    elif column == 1:
        add(ALONE, 1, LOW_FIRST, pass_on="own")
        add(DIRECT, 0, LOW_FIRST, right=LOW)
        add(DIRECT, "relay", LOW_FIRST, up=every, pass_on="none")
        add(SECOND, 2, LOW_FIRST, left=every)
        add(THIRD[:2], 3, LOW)
        add(THIRD[:2], 3, HIGH)
    elif column == 2:
        add(ALONE, 2, LOW_FIRST, pass_on="own")
        add(DIRECT, 1, LOW_FIRST, right=every)
        add(DIRECT, "relay", HIGH_FIRST, up=every, pass_on="none")
        add(SECOND, 3, HIGH_FIRST, left=HIGH)
        add([8.7, 10.1], 0, LOW)
        add([8.7, 10.1], 0, HIGH)
    else:
        add(DIRECT, 3, LOW_FIRST, right=every, pass_on="own_wait")
        add(DIRECT, 2, LOW_FIRST)
        add(DIRECT, 0, HIGH_FIRST, left=HIGH)
        add([8.7, 10.1, 11.5, 12.9], 1, LOW_FIRST)
    return sorted(events, key=lambda event: event[0])


def gather_kernel(
    x_ref, wq_ref, wk_ref, wv_ref, pk_ref, pv_ref,
    q_ref, k_ref, v_ref, kv_ref,
    xbuf, wq, wk, wv, acc, relay,
    w_sem, local_sem, x_send, x_recv,
    right_send, left_send, up_send, relay_send, right_fwd, left_fwd, pair_send,
    slot_recv, relay_recv, pair_recv,
):
    section = lax.axis_index("section")
    y = lax.axis_index("head")
    core = lax.rem(section, 2)
    x = lax.rem(lax.div(section, 2), COLUMNS)
    z = lax.div(section, 2 * COLUMNS)

    def section_at(layer, column, kind):
        return (layer * COLUMNS + column) * 2 + kind

    right = section_at(z, lax.rem(x + 1, COLUMNS), core)
    left = section_at(z, lax.rem(x + COLUMNS - 1, COLUMNS), core)
    above = section_at(lax.rem(z + 1, LAYERS), x, core)
    below = section_at(lax.rem(z + LAYERS - 1, LAYERS), x, core)
    pair = section_at(z, x, 1 - core)
    y_up = lax.rem(y + 1, RING)
    y_down = lax.rem(y + RING - 1, RING)

    def block_at(hop):
        return lax.rem(y + hop + RING, RING)

    visits = [0, -1, 1, -2, 2, -3, 3, 4]

    def weight_copies(hop):
        start = pl.multiple_of(block_at(hop) * 512, 512)
        rows = pl.ds(start, 512)
        at = visits.index(hop)
        return [
            pltpu.make_async_copy(source.at[rows], target.at[rows], w_sem.at[at, index])
            for index, (source, target) in enumerate(((wq_ref, wq), (wk_ref, wk), (wv_ref, wv)))
        ]

    own_x = pltpu.make_async_copy(x_ref, xbuf.at[y], local_sem.at[0])
    own_x.start()
    for copy in weight_copies(0):
        copy.start()

    barrier = pltpu.get_barrier_semaphore()
    for peer in (right, left, above, below, pair):
        pl.semaphore_signal(barrier, inc=1, device_id=(peer, y), device_id_type=MESH)
    for peer in (y_up, y_down):
        pl.semaphore_signal(barrier, inc=1, device_id=(section, peer), device_id_type=MESH)
    for hop in visits[1:]:
        for copy in weight_copies(hop):
            copy.start()
    own_k = pltpu.make_async_copy(pk_ref, kv_ref.at[8, 0], local_sem.at[1])
    own_v = pltpu.make_async_copy(pv_ref, kv_ref.at[8, 1], local_sem.at[2])
    own_k.start()
    own_v.start()
    pl.semaphore_wait(barrier, 7)

    def remote(source, target, send, recv, device):
        return pltpu.make_async_remote_copy(
            src_ref=source, dst_ref=target, send_sem=send, recv_sem=recv,
            device_id=device, device_id_type=MESH,
        )

    def x_copy(way, hop, half):
        origin = block_at(-hop if way == 0 else hop)
        rows = pl.ds(half * HALF, HALF)
        source = x_ref.at[rows] if hop == 0 else xbuf.at[origin, rows]
        return remote(
            source, xbuf.at[origin, rows],
            x_send.at[way, hop * 2 + half], x_recv.at[way, hop * 2 + half],
            (section, y_up if way == 0 else y_down),
        )

    def x_arrival(way, hop, half):
        origin = block_at(-hop - 1 if way == 0 else hop + 1)
        rows = pl.ds(half * HALF, HALF)
        return remote(
            xbuf.at[origin, rows], xbuf.at[origin, rows],
            x_send.at[way, hop * 2 + half], x_recv.at[way, hop * 2 + half],
            (section, y_up if way == 0 else y_down),
        )

    def x_sent(way, hop, half):
        return hop < 3 or half == way

    def own_piece(piece):
        return (pk_ref if piece % 2 == 0 else pv_ref).at[rows_of(piece)]

    def slot_piece(column, kind, piece):
        return kv_ref.at[column * 2 + kind, piece % 2, rows_of(piece)]

    def relay_piece(piece):
        return relay.at[piece % 2, rows_of(piece)]

    def send_right(piece):
        return remote(
            own_piece(piece), slot_piece(x, core, piece),
            right_send.at[piece], slot_recv.at[x, piece], (right, y),
        )

    def send_left(piece, column):
        if column == 0:
            return remote(
                own_piece(piece), slot_piece(0, core, piece),
                left_send.at[piece], slot_recv.at[0, piece], (left, y),
            )
        return remote(
            own_piece(piece), relay_piece(piece),
            left_send.at[piece], relay_recv.at[piece], (left, y),
        )

    def send_up(piece):
        return remote(
            own_piece(piece), slot_piece(x, core, piece),
            up_send.at[piece], slot_recv.at[x, piece], (above, y),
        )

    def send_relay(piece, column):
        return remote(
            relay_piece(piece), slot_piece(column + 1, core, piece),
            relay_send.at[piece], slot_recv.at[column + 1, piece], (above, y),
        )

    def forward(slot, piece, to_right):
        return remote(
            slot_piece(slot, core, piece), slot_piece(slot, core, piece),
            (right_fwd if to_right else left_fwd).at[piece], slot_recv.at[slot, piece],
            (right if to_right else left, y),
        )

    def hand_over(slot, piece):
        return remote(
            slot_piece(slot, core, piece), slot_piece(slot, core, piece),
            pair_send.at[slot, piece], pair_recv.at[slot, piece], (pair, y),
        )

    def hand_own(piece):
        return remote(
            own_piece(piece), slot_piece(x, 0, piece),
            pair_send.at[x, piece], pair_recv.at[x, piece], (pair, y),
        )

    for half in range(2):
        for way in range(2):
            x_copy(way, 0, half).start()
    for column in range(COLUMNS):

        @pl.when(x == column)
        def _():
            order = HIGH_FIRST if column in (0, 3) else LOW_FIRST
            for index in range(4):
                send_left(order[index], column).start()
                if column < 3:
                    send_right(index).start()
                else:
                    send_up(index).start()

    @pl.when((core == 1) & (x < 3))
    def _():
        for piece in range(4):
            send_up(piece).start()

    @pl.when(core == 0)
    def _():
        for piece in range(4):
            hand_own(piece).start()

    def handle(column, event):
        _, slot, piece, to_right, to_left, to_up, pass_on = event

        def run():
            if slot == "relay":
                remote(
                    relay_piece(piece), relay_piece(piece),
                    relay_send.at[piece], relay_recv.at[piece], (above, y),
                ).wait_recv()
                send_relay(piece, column).start()
                return
            remote(
                slot_piece(slot, core, piece), slot_piece(slot, core, piece),
                pair_send.at[slot, piece], slot_recv.at[slot, piece], (pair, y),
            ).wait_recv()
            if to_right:
                forward(slot, piece, True).start()
            if to_left:
                forward(slot, piece, False).start()
            if pass_on == "both" or pass_on == "own":
                hand_over(slot, piece).start()
            if pass_on == "own_wait":

                @pl.when(core == 1)
                def _():
                    hand_over(slot, piece).start()

        if pass_on == "own":
            pl.when(core == 1)(run)
        else:
            run()

    schedules = [arrivals(column) for column in range(COLUMNS)]

    def prefixes(until):
        for column in range(COLUMNS):
            due = [event for event in schedules[column] if event[0] <= until]
            if not due:
                continue
            schedules[column] = schedules[column][len(due) :]

            @pl.when(x == column)
            def _():
                for event in due:
                    handle(column, event)

    def project(hop):
        start = pl.multiple_of(block_at(hop) * 512, 512)
        rows = pl.ds(start, 512)
        for copy in weight_copies(hop):
            copy.wait()
        block = xbuf[block_at(hop)]
        for weight, first, size in ((wq, 0, 512), (wk, 512, 128), (wv, 640, 128)):
            part = jnp.dot(block, weight[rows, :], preferred_element_type=jnp.float32)
            if hop == 0:
                acc[:, first : first + size] = part
            else:
                acc[:, first : first + size] += part

    own_x.wait()
    project(0)
    times = {(0, 0): 4.2, (0, 1): 5.6, (1, 0): 7.3, (1, 1): 8.7, (2, 0): 10.4, (2, 1): 11.8}
    for hop in range(3):
        for half in range(2):
            for way in range(2):
                x_arrival(way, hop, half).wait_recv()
                if x_sent(way, hop + 1, half):
                    x_copy(way, hop + 1, half).start()
            prefixes(times[hop, half])
        project(-(hop + 1))
        project(hop + 1)
    prefixes(12.5)
    for way in range(2):
        x_arrival(way, 3, way).wait_recv()
    project(4)
    prefixes(99.0)
    for group in range(4):
        q_ref[group * 128 : (group + 1) * 128, :] = acc[:, group * 128 : (group + 1) * 128].astype(jnp.bfloat16)
    k_ref[...] = acc[:, 512:640].astype(jnp.bfloat16)
    v_ref[...] = acc[:, 640:768].astype(jnp.bfloat16)

    own_k.wait()
    own_v.wait()
    for slot in range(COLUMNS):
        for piece in range(4):
            remote(
                slot_piece(slot, 1 - core, piece), slot_piece(slot, 1 - core, piece),
                pair_send.at[slot, piece], pair_recv.at[slot, piece], (pair, y),
            ).wait_recv()

    for hop in range(4):
        for half in range(2):
            for way in range(2):
                if x_sent(way, hop, half):
                    x_copy(way, hop, half).wait_send()
    for column in range(COLUMNS):

        @pl.when(x == column)
        def _():
            for piece in range(4):
                send_left(piece, column).wait_send()
                if column < 3:
                    send_right(piece).wait_send()
                    send_relay(piece, column).wait_send()
                else:
                    send_up(piece).wait_send()
            for _, slot, piece, to_right, to_left, _, pass_on in arrivals(column):
                if to_right:
                    forward(slot, piece, True).wait_send()
                if to_left:
                    forward(slot, piece, False).wait_send()
                if pass_on == "both":
                    hand_over(slot, piece).wait_send()

    @pl.when((core == 1) & (x < 3))
    def _():
        for piece in range(4):
            send_up(piece).wait_send()

    for piece in range(4):
        hand_own(piece).wait_send()


def gather(slice_rows, w_query, w_key, w_value, prefix_keys, prefix_values):
    bf16, f32 = jnp.bfloat16, jnp.float32
    dma = pltpu.SemaphoreType.DMA
    anywhere = pl.BlockSpec(memory_space=pl.ANY)
    vmem = pl.BlockSpec(memory_space=pltpu.VMEM)
    return pl.pallas_call(
        gather_kernel,
        out_shape=(
            pltpu.VMEM((512, HEAD_DIM), bf16),
            pltpu.VMEM((128, HEAD_DIM), bf16),
            pltpu.VMEM((128, HEAD_DIM), bf16),
            pltpu.VMEM((9, 2, 512, HEAD_DIM), bf16),
        ),
        in_specs=[anywhere] * 6,
        out_specs=(vmem,) * 4,
        scratch_shapes=[
            pltpu.VMEM((RING, 128, 512), bf16),
            pltpu.VMEM((4096, 512), bf16),
            pltpu.VMEM((4096, 128), bf16),
            pltpu.VMEM((4096, 128), bf16),
            pltpu.VMEM((128, 768), f32),
            pltpu.VMEM((2, 512, HEAD_DIM), bf16),
            dma((8, 3)), dma((3,)), dma((2, 8)), dma((2, 8)),
            dma((4,)), dma((4,)), dma((4,)), dma((4,)), dma((4,)), dma((4,)), dma((4, 4)),
            dma((4, 4)), dma((4,)), dma((4, 4)),
        ],
        compiler_params=pltpu.CompilerParams(
            collective_id=0, has_side_effects=True, vmem_limit_bytes=32 * 1024 * 1024
        ),
        name="gather",
    )(slice_rows, w_query, w_key, w_value, prefix_keys, prefix_values)


def scores_of(keys, queries):
    return lax.dot_general(
        keys, queries, (((1,), (1,)), ((), ())), preferred_element_type=jnp.float32
    )


def weigh(values, weights):
    return lax.dot_general(
        values, weights, (((0,), (0,)), ((), ())), preferred_element_type=jnp.float32
    )


def attend_kernel(pb_ref, q_ref, k_ref, v_ref, kv_ref, out_ref, scores, m_ref, l_ref, o_ref):
    section = lax.axis_index("section")
    factor = math.log2(math.e) / math.sqrt(HEAD_DIM)
    never = 1e30
    queries = q_ref[...]

    def slot_of(offset):
        return 8 if offset == 0 else lax.rem(section - offset + 64, 8)

    key_row = lax.broadcasted_iota(jnp.int32, (128, 512), 0)
    query_row = lax.broadcasted_iota(jnp.int32, (128, 512), 1) % 128
    own = jnp.where(key_row <= query_row, scores_of(k_ref[...], queries), -never)
    top = jnp.max(own, axis=0, keepdims=True)
    for offset in range(REACH + 1):
        part = scores_of(kv_ref[slot_of(offset), 0, :BLOCK, :], queries)
        scores[offset] = part
        peak = jnp.max(part, axis=0, keepdims=True)
        top = jnp.maximum(top, jnp.where(section >= offset, peak, -never))
    weights = jnp.exp2((own - top) * factor)
    total = jnp.sum(weights, axis=0, keepdims=True)
    result = weigh(v_ref[...], weights.astype(jnp.bfloat16))
    for offset in range(REACH + 1):
        shift = jnp.where(section >= offset, top, never)
        weights = jnp.exp2((scores[offset] - shift) * factor)
        total += jnp.sum(weights, axis=0, keepdims=True)
        result += weigh(kv_ref[slot_of(offset), 1, :BLOCK, :], weights.astype(jnp.bfloat16))
    m_ref[...] = top
    l_ref[...] = total
    o_ref[...] = result

    for offset in range(REACH + 1):
        blocks = pb_ref[jnp.maximum(section - offset, 0)]

        @pl.when((section >= offset) & (blocks > 1))
        def _():
            part = scores_of(kv_ref[slot_of(offset), 0, BLOCK:, :], queries)
            before = m_ref[...]
            after = jnp.maximum(before, jnp.max(part, axis=0, keepdims=True))
            keep = jnp.exp2((before - after) * factor)
            weights = jnp.exp2((part - after) * factor)
            m_ref[...] = after
            l_ref[...] = l_ref[...] * keep + jnp.sum(weights, axis=0, keepdims=True)
            o_ref[...] = o_ref[...] * keep + weigh(
                kv_ref[slot_of(offset), 1, BLOCK:, :], weights.astype(jnp.bfloat16)
            )

    final = o_ref[...] / l_ref[...]
    for group in range(4):
        part = final[:, group * 128 : (group + 1) * 128]
        out_ref[:, group * 128 : (group + 1) * 128] = part.T.astype(jnp.bfloat16)


def attend(prefix_blocks, queries, own_keys, own_values, kv):
    vmem = pl.BlockSpec(memory_space=pltpu.VMEM)
    return pl.pallas_call(
        attend_kernel,
        out_shape=jax.ShapeDtypeStruct((128, 512), jnp.bfloat16),
        in_specs=[pl.BlockSpec(memory_space=pltpu.SMEM)] + [vmem] * 4,
        out_specs=vmem,
        scratch_shapes=[
            pltpu.VMEM((REACH + 1, BLOCK, 512), jnp.float32),
            pltpu.VMEM((1, 512), jnp.float32),
            pltpu.VMEM((1, 512), jnp.float32),
            pltpu.VMEM((HEAD_DIM, 512), jnp.float32),
        ],
        compiler_params=pltpu.CompilerParams(vmem_limit_bytes=24 * 1024 * 1024),
        name="attend",
    )(prefix_blocks, queries, own_keys, own_values, kv)


def on_device(slice_rows, w_query, w_key, w_value, prefix_keys, prefix_values, prefix_blocks):
    queries, own_keys, own_values, kv = gather(
        slice_rows, w_query, w_key, w_value, prefix_keys, prefix_values
    )
    return attend(prefix_blocks, queries, own_keys, own_values, kv)


def solution(mesh):
    in_specs = (
        P("section", "head"),
        P(None, "head"),
        P(None, "head"),
        P(None, "head"),
        P("section", "head"),
        P("section", "head"),
        P(),
    )
    out_specs = P("section", "head")
    return jax.shard_map(
        on_device, mesh=mesh, in_specs=in_specs, out_specs=out_specs, check_vma=False
    )
```

```python
import functools
import math

import jax
import jax.numpy as jnp
from jax import lax
from jax.experimental import pallas as pl
from jax.experimental.pallas import tpu as pltpu
from jax.sharding import PartitionSpec as P

HEAD_DIM = 128
BLOCK = 256
REACH = 7
COLUMNS = 4
LAYERS = 8
RING = 8
MESH = pl.DeviceIdType.MESH

LOW_FIRST = [0, 1, 2, 3]
HIGH_FIRST = [2, 3, 0, 1]
LOW, HIGH = (0, 1), (2, 3)
PIECES = 4
PIECE = 128 // PIECES


def rows_of(piece):
    return pl.ds((piece // 2) * BLOCK, BLOCK)


def steps(first, each=1.4):
    return [first + each * index for index in range(4)]


def arrivals(column):
    events = []

    def add(times, slot, order=LOW_FIRST, kinds=(0, 1), right=(), left=(), up=False, pair=True):
        for kind in kinds:
            for time, piece in zip(times, order):
                events.append(
                    dict(
                        time=time + 0.3 * kind, slot=slot, kind=kind, piece=piece,
                        right=piece in right, left=piece in left, up=up, pair=pair,
                        prev=slot != "relay" and slot >= column,
                    )
                )

    every = LOW + HIGH
    direct, relayed = steps(4.2), steps(6.6)
    if column < 3:
        add(steps(4.0, 0.7), column, kinds=(1,))
        add(direct, "relay", HIGH_FIRST if column == 2 else LOW_FIRST, up=True, pair=False)
    if column == 0:
        add(relayed, 1)
        add(steps(7.4), 3, right=LOW)
        add(steps(9.0), 2)
    elif column == 1:
        add(direct, 0, right=LOW)
        add(relayed, 2, left=every)
        add([9.8, 11.2], 3, LOW)
        add([9.0, 10.4], 3, HIGH)
    elif column == 2:
        add(direct, 1, right=every)
        add(relayed, 3, HIGH_FIRST, left=HIGH)
        add([8.0, 9.4], 0, LOW)
        add([8.0, 9.4], 0, HIGH)
    else:
        add(steps(4.8), 3, kinds=(0,), right=every, pair=False)
        add(steps(4.8), 3, kinds=(1,), right=every)
        add(direct, 2)
        add(direct, 0, HIGH_FIRST, left=HIGH)
        add(steps(8.0), 1)
    return sorted(events, key=lambda event: event["time"])


def gather_kernel(
    x_ref, wq_ref, wk_ref, wv_ref, pk_ref, pv_ref,
    q_ref, k_ref, v_ref, kv_ref,
    xbuf, xother, wq, wk, wv, acc, relay,
    w_sem, local_sem, x_send, x_recv, x_pair_send, x_pair_recv,
    right_send, left_send, up_send, own_send, relay_send, right_fwd, left_fwd, pair_send,
    slot_recv, relay_recv, pair_recv, ready,
):
    section = lax.axis_index("section")
    y = lax.axis_index("head")
    core = lax.rem(section, 2)
    x = lax.rem(lax.div(section, 2), COLUMNS)
    z = lax.div(section, 2 * COLUMNS)

    def at(layer, column, kind, ring=None):
        return ((layer * COLUMNS + column) * 2 + kind, y if ring is None else ring)

    x_right, x_left = lax.rem(x + 1, COLUMNS), lax.rem(x + COLUMNS - 1, COLUMNS)
    z_above, z_below = lax.rem(z + 1, LAYERS), lax.rem(z + LAYERS - 1, LAYERS)
    y_up, y_down = lax.rem(y + 1, RING), lax.rem(y + RING - 1, RING)
    right, left = at(z, x_right, 1), at(z, x_left, 1)
    above = at(z_above, x, 1)
    ways = (at(z, x, 1, y_up), at(z, x, 1, y_down))
    pair = at(z, x, 1 - core)

    def block_at(hop):
        return lax.rem(y + hop + RING, RING)

    visits = [0, -1, 1, -2, 2, -3, 3, 4]

    def weight_copies(hop):
        start = pl.multiple_of(block_at(hop) * 512, 512)
        rows = pl.ds(start, 512)
        place = visits.index(hop)
        return [
            pltpu.make_async_copy(source.at[rows], target.at[rows], w_sem.at[place, index])
            for index, (source, target) in enumerate(((wq_ref, wq), (wk_ref, wk), (wv_ref, wv)))
        ]

    def project(hop):
        start = pl.multiple_of(block_at(hop) * 512, 512)
        rows = pl.ds(start, 512)
        for copy in weight_copies(hop):
            copy.wait()
        block = xbuf[block_at(hop)]
        for weight, first, size in ((wq, 0, 512), (wk, 512, 128), (wv, 640, 128)):
            part = jnp.dot(block, weight[rows, :], preferred_element_type=jnp.float32)
            if hop == 0:
                acc[:, first : first + size] = part
            else:
                acc[:, first : first + size] += part

    def remote(source, target, send, recv, device):
        return pltpu.make_async_remote_copy(
            src_ref=source, dst_ref=target, send_sem=send, recv_sem=recv,
            device_id=device, device_id_type=MESH,
        )

    own_x = pltpu.make_async_copy(x_ref, xbuf.at[y], local_sem.at[0])
    own_k = pltpu.make_async_copy(pk_ref, kv_ref.at[8, 0], local_sem.at[1])
    own_v = pltpu.make_async_copy(pv_ref, kv_ref.at[8, 1], local_sem.at[2])
    own_x.start()
    for copy in weight_copies(0):
        copy.start()

    def tell(semaphore, device):
        pl.semaphore_signal(semaphore, inc=1, device_id=device, device_id_type=MESH)

    barrier = pltpu.get_barrier_semaphore()

    @pl.when(core == 1)
    def _():
        for kind in range(2):
            for device in (
                at(z, x, kind, y_up), at(z, x, kind, y_down),
                at(z, x_right, kind), at(z, x_left, kind),
            ):
                tell(barrier, device)

    tell(barrier, pair)

    @pl.when((z < LAYERS - 1) & ((core == 1) | (x == 3)))
    def _():
        tell(barrier, above)

    for hop in visits[1:]:
        for copy in weight_copies(hop):
            copy.start()
    own_k.start()
    own_v.start()
    below_count = jnp.where((core == 1) & (z > 0), jnp.where(x == 3, 2, 1), 0)
    pl.semaphore_wait(barrier, 5 + below_count)

    @pl.when((core == 1) & (z > 0))
    def _():
        tell(ready, at(z_below, x, 1))

        @pl.when(x == 3)
        def _():
            tell(ready, at(z_below, x, 0))

    def rows_at(piece):
        return pl.ds(piece * PIECE, PIECE)

    def x_own(way, piece, kind):
        target = xother if kind == 0 else xbuf
        return remote(
            x_ref.at[rows_at(piece)], target.at[y, rows_at(piece)],
            x_send.at[way, kind, piece], x_recv.at[way, kind, piece], ways[way],
        )

    def x_origin(way, hop):
        return block_at(-hop - 1 if way == 0 else hop + 1)

    def x_piece(way, hop, piece, kind):
        return (xother if kind == 0 else xbuf).at[x_origin(way, hop), rows_at(piece)]

    def x_arrival(way, hop, piece, kind):
        here = x_piece(way, hop, piece, kind)
        index = hop * PIECES + piece
        return remote(here, here, x_send.at[way, kind, index], x_recv.at[way, kind, index], ways[way])

    def x_forward(way, hop, piece, kind):
        here = x_piece(way, hop, piece, kind)
        index = (hop + 1) * PIECES + piece
        return remote(here, here, x_send.at[way, kind, index], x_recv.at[way, kind, index], ways[way])

    def x_hand(way, hop, piece):
        index = hop * PIECES + piece
        rows = rows_at(piece)
        return remote(
            xother.at[x_origin(way, hop), rows], xbuf.at[x_origin(way, hop), rows],
            x_pair_send.at[way, index], x_pair_recv.at[way, index], pair,
        )

    def travels(way, hop, piece):
        return hop < 3 or (hop == 3 and piece // (PIECES // 2) == way)

    def own_piece(piece):
        return (pk_ref if piece % 2 == 0 else pv_ref).at[rows_of(piece)]

    def slot_piece(column, kind, piece):
        return kv_ref.at[column * 2 + kind, piece % 2, rows_of(piece)]

    def relay_piece(kind, piece):
        return relay.at[kind, piece % 2, rows_of(piece)]

    def send_right(kind, piece, column):
        return remote(
            own_piece(piece), slot_piece(column, kind, piece),
            right_send.at[piece], slot_recv.at[column * 2 + kind, piece], right,
        )

    def send_left(kind, piece, column):
        if column == 0:
            target, arrived = slot_piece(0, kind, piece), slot_recv.at[kind, piece]
        else:
            target, arrived = relay_piece(kind, piece), relay_recv.at[kind, piece]
        return remote(own_piece(piece), target, left_send.at[piece], arrived, left)

    def send_up(kind, piece):
        if kind == 0:
            target, arrived = relay_piece(0, piece), relay_recv.at[0, piece]
        else:
            target, arrived = slot_piece(x, 1, piece), slot_recv.at[x * 2 + 1, piece]
        return remote(own_piece(piece), target, up_send.at[piece], arrived, above)

    def send_pair(piece):
        return remote(
            own_piece(piece), slot_piece(x, 0, piece),
            own_send.at[piece], pair_recv.at[x * 2, piece], pair,
        )

    def first_sends(kind, column):
        order = HIGH_FIRST if column in (0, 3) else LOW_FIRST
        for index in range(4):
            piece = order[index]
            yield column > 0, functools.partial(send_left, kind, piece, column)
            if column < 3:
                yield False, functools.partial(send_right, kind, index, column)

    def source_of(event, column):
        kind, piece = event["kind"], event["piece"]
        if event["slot"] == "relay" or (column == 3 and event["slot"] == 3 and kind == 0):
            return relay_piece(kind, piece), relay_recv.at[kind, piece]
        slot = event["slot"]
        return slot_piece(slot, kind, piece), slot_recv.at[slot * 2 + kind, piece]

    def sends_of(event, column):
        kind, piece, slot = event["kind"], event["piece"], event["slot"]
        source, _ = source_of(event, column)
        copies = []
        if event["up"]:
            return [
                remote(
                    source, slot_piece(column + 1, kind, piece), relay_send.at[kind, piece],
                    slot_recv.at[(column + 1) * 2 + kind, piece], above,
                )
            ]
        target, arrived = slot_piece(slot, kind, piece), slot_recv.at[slot * 2 + kind, piece]
        if event["right"]:
            copies.append(remote(source, target, right_fwd.at[kind, piece], arrived, right))
        if event["left"]:
            copies.append(remote(source, target, left_fwd.at[kind, piece], arrived, left))
        if event["pair"]:
            copies.append(
                remote(
                    source, target, pair_send.at[slot * 2 + kind, piece],
                    pair_recv.at[slot * 2 + kind, piece], pair,
                )
            )
        return copies

    def guarded(condition, run):
        if condition is None:
            run()
        else:
            pl.when(condition)(run)

    def start_first(kind):
        for piece in range(PIECES):
            for way in range(2):
                x_own(way, piece, kind).start()
        for column in range(COLUMNS):

            @pl.when(x == column)
            def _():
                plain = [make for needs, make in first_sends(kind, column) if not needs]
                needing = [make for needs, make in first_sends(kind, column) if needs]
                if needing:

                    @pl.when(z < LAYERS - 1)
                    def _():
                        for make in needing:
                            make().start()

                for make in plain:
                    make().start()

    def finish_first(kind):
        for piece in range(PIECES):
            for way in range(2):
                x_own(way, piece, kind).wait_send()
        for column in range(COLUMNS):

            @pl.when(x == column)
            def _():
                for needs, make in first_sends(kind, column):
                    if not needs:
                        make().wait_send()
                if column > 0:

                    @pl.when(z < LAYERS - 1)
                    def _():
                        for needs, make in first_sends(kind, column):
                            if needs:
                                make().wait_send()

    @pl.when(z == 0)
    def _():
        for column in range(COLUMNS):

            @pl.when(x == column)
            def _():
                for slot in range(column * 2 + 2, COLUMNS * 2):
                    kv_ref[slot] = jnp.zeros((2, 512, HEAD_DIM), jnp.bfloat16)

                @pl.when(core == 0)
                def _():
                    kv_ref[column * 2 + 1] = jnp.zeros((2, 512, HEAD_DIM), jnp.bfloat16)

    @pl.when(core == 0)
    def _():
        start_first(0)
        for piece in range(4):
            send_pair(piece).start()
        own_x.wait()
        project(0)

        @pl.when((x == 3) & (z < LAYERS - 1))
        def _():
            pl.semaphore_wait(ready, 1)
            for piece in range(4):
                send_up(0, piece).start()

        for hop in range(4):
            for way in range(2):
                for piece in range(PIECES):
                    if travels(way, hop, piece):
                        x_hand(way, hop, piece).wait_recv()
                if hop < 3:
                    project(-hop - 1 if way == 0 else hop + 1)
        project(4)
        for column in range(COLUMNS):

            @pl.when(x == column)
            def _():
                def take(slot, kind):
                    for piece in range(4):
                        here = slot_piece(slot, kind, piece)
                        index = slot * 2 + kind
                        remote(
                            here, here, pair_send.at[index, piece], pair_recv.at[index, piece], pair
                        ).wait_recv()

                for slot in range(column):
                    for kind in range(2):
                        take(slot, kind)

                @pl.when(z > 0)
                def _():
                    take(column, 1)
                    for slot in range(column + 1, COLUMNS):
                        for kind in range(2):
                            take(slot, kind)

        finish_first(0)
        for piece in range(4):
            send_pair(piece).wait_send()

        @pl.when((x == 3) & (z < LAYERS - 1))
        def _():
            for piece in range(4):
                send_up(0, piece).wait_send()

    schedules = [arrivals(column) for column in range(COLUMNS)]

    def handle(event, column):
        source, arrived = source_of(event, column)

        def run():
            remote(source, source, pair_send.at[0, 0], arrived, pair).wait_recv()
            if event["up"]:

                @pl.when(z > 0)
                def _():
                    for copy in sends_of(event, column):
                        copy.start()

            else:
                for copy in sends_of(event, column):
                    copy.start()

        guarded(condition_of(event), run)

    def condition_of(event):
        return z < LAYERS - 1 if event["up"] else z > 0 if event["prev"] else None

    def prefixes(until):
        for column in range(COLUMNS):
            due = [event for event in schedules[column] if event["time"] <= until]
            if not due:
                continue
            schedules[column] = schedules[column][len(due) :]

            @pl.when(x == column)
            def _():
                for event in due:
                    handle(event, column)

    def lowest_goes_up():
        @pl.when(z == 0)
        def _():
            pl.semaphore_wait(ready, 1)
            for piece in range(4):
                send_up(1, piece).start()
            for column in range(COLUMNS - 1):

                @pl.when(x == column)
                def _():
                    for event in arrivals(column):
                        if event["up"]:
                            for copy in sends_of(event, column):
                                copy.start()

    @pl.when(core == 1)
    def _():
        start_first(1)

        @pl.when((z > 0) & (z < LAYERS - 1))
        def _():
            pl.semaphore_wait(ready, 1)
            for piece in range(4):
                send_up(1, piece).start()

        own_x.wait()
        project(0)
        clock = {0: 3.5, 1: 5.9, 2: 8.3, 3: 10.7}
        for hop in range(4):
            for piece in range(PIECES):
                if hop == 3 and piece >= PIECES // 2:
                    continue
                for kind in range(2):
                    for way in range(2):
                        this = piece if hop < 3 or way == 0 else piece + PIECES // 2
                        x_arrival(way, hop, this, kind).wait_recv()
                        if travels(way, hop + 1, this):
                            x_forward(way, hop, this, kind).start()
                        if kind == 0:
                            x_hand(way, hop, this).start()
                prefixes(clock[hop] + 2.4 / PIECES * piece)
                if hop > 0 and piece == 0:
                    project(-hop)
                if hop > 0 and piece == 1:
                    project(hop)
                if hop == 2 and piece == 1:
                    lowest_goes_up()
        project(4)
        prefixes(99.0)
        for piece in range(4):
            here = slot_piece(x, 0, piece)
            remote(here, here, pair_send.at[0, 0], pair_recv.at[x * 2, piece], pair).wait_recv()

        finish_first(1)
        for hop in range(4):
            for piece in range(PIECES):
                for way in range(2):
                    for kind in range(2):
                        if travels(way, hop + 1, piece):
                            x_forward(way, hop, piece, kind).wait_send()
                    if travels(way, hop, piece):
                        x_hand(way, hop, piece).wait_send()

        @pl.when(z < LAYERS - 1)
        def _():
            for piece in range(4):
                send_up(1, piece).wait_send()

        for column in range(COLUMNS):

            @pl.when(x == column)
            def _():
                events = arrivals(column)
                for event in events:
                    if not event["up"] and not event["prev"]:
                        for copy in sends_of(event, column):
                            copy.wait_send()

                @pl.when(z > 0)
                def _():
                    for event in events:
                        if event["prev"]:
                            for copy in sends_of(event, column):
                                copy.wait_send()

                @pl.when(z < LAYERS - 1)
                def _():
                    for event in events:
                        if event["up"]:
                            for copy in sends_of(event, column):
                                copy.wait_send()

    for group in range(4):
        q_ref[group * 128 : (group + 1) * 128, :] = acc[:, group * 128 : (group + 1) * 128].astype(jnp.bfloat16)
    k_ref[...] = acc[:, 512:640].astype(jnp.bfloat16)
    v_ref[...] = acc[:, 640:768].astype(jnp.bfloat16)
    own_k.wait()
    own_v.wait()


def gather(slice_rows, w_query, w_key, w_value, prefix_keys, prefix_values):
    bf16, f32 = jnp.bfloat16, jnp.float32
    dma = pltpu.SemaphoreType.DMA
    anywhere = pl.BlockSpec(memory_space=pltpu.HBM)
    vmem = pl.BlockSpec(memory_space=pltpu.VMEM)
    return pl.pallas_call(
        gather_kernel,
        out_shape=(
            pltpu.VMEM((512, HEAD_DIM), bf16),
            pltpu.VMEM((128, HEAD_DIM), bf16),
            pltpu.VMEM((128, HEAD_DIM), bf16),
            pltpu.VMEM((9, 2, 512, HEAD_DIM), bf16),
        ),
        in_specs=[anywhere] * 6,
        out_specs=(vmem,) * 4,
        scratch_shapes=[
            pltpu.VMEM((RING, 128, 512), bf16),
            pltpu.VMEM((RING, 128, 512), bf16),
            pltpu.VMEM((4096, 512), bf16),
            pltpu.VMEM((4096, 128), bf16),
            pltpu.VMEM((4096, 128), bf16),
            pltpu.VMEM((128, 768), f32),
            pltpu.VMEM((2, 2, 512, HEAD_DIM), bf16),
            dma((8, 3)), dma((3,)),
            dma((2, 2, 4 * PIECES)), dma((2, 2, 4 * PIECES)), dma((2, 4 * PIECES)), dma((2, 4 * PIECES)),
            dma((4,)), dma((4,)), dma((4,)), dma((4,)),
            dma((2, 4)), dma((2, 4)), dma((2, 4)), dma((8, 4)),
            dma((8, 4)), dma((2, 4)), dma((8, 4)), pltpu.SemaphoreType.REGULAR,
        ],
        compiler_params=pltpu.CompilerParams(
            collective_id=0, has_side_effects=True, vmem_limit_bytes=58 * 1024 * 1024
        ),
        name="gather",
    )(slice_rows, w_query, w_key, w_value, prefix_keys, prefix_values)


def scores_of(keys, queries):
    return lax.dot_general(
        keys, queries, (((1,), (1,)), ((), ())), preferred_element_type=jnp.float32
    )


def weigh(values, weights):
    return lax.dot_general(
        values, weights, (((0,), (0,)), ((), ())), preferred_element_type=jnp.float32
    )


def attend_kernel(pb_ref, q_ref, k_ref, v_ref, kv_ref, out_ref, scores, m_ref, l_ref, o_ref):
    section = lax.axis_index("section")
    factor = math.log2(math.e) / math.sqrt(HEAD_DIM)
    never = 1e30
    queries = q_ref[...]

    def slot_of(offset):
        return 8 if offset == 0 else lax.rem(section - offset + 64, 8)

    key_row = lax.broadcasted_iota(jnp.int32, (128, 512), 0)
    query_row = lax.broadcasted_iota(jnp.int32, (128, 512), 1) % 128
    own = jnp.where(key_row <= query_row, scores_of(k_ref[...], queries), -never)
    top = jnp.max(own, axis=0, keepdims=True)
    for offset in range(REACH + 1):
        part = scores_of(kv_ref[slot_of(offset), 0, :BLOCK, :], queries)
        scores[offset] = part
        peak = jnp.max(part, axis=0, keepdims=True)
        top = jnp.maximum(top, jnp.where(section >= offset, peak, -never))
    weights = jnp.exp2((own - top) * factor)
    total = jnp.sum(weights, axis=0, keepdims=True)
    result = weigh(v_ref[...], weights.astype(jnp.bfloat16))
    for offset in range(REACH + 1):
        shift = jnp.where(section >= offset, top, never)
        weights = jnp.exp2((scores[offset] - shift) * factor)
        total += jnp.sum(weights, axis=0, keepdims=True)
        result += weigh(kv_ref[slot_of(offset), 1, :BLOCK, :], weights.astype(jnp.bfloat16))
    m_ref[...] = top
    l_ref[...] = total
    o_ref[...] = result

    for offset in range(REACH + 1):
        blocks = pb_ref[jnp.maximum(section - offset, 0)]

        @pl.when((section >= offset) & (blocks > 1))
        def _():
            part = scores_of(kv_ref[slot_of(offset), 0, BLOCK:, :], queries)
            before = m_ref[...]
            after = jnp.maximum(before, jnp.max(part, axis=0, keepdims=True))
            keep = jnp.exp2((before - after) * factor)
            weights = jnp.exp2((part - after) * factor)
            m_ref[...] = after
            l_ref[...] = l_ref[...] * keep + jnp.sum(weights, axis=0, keepdims=True)
            o_ref[...] = o_ref[...] * keep + weigh(
                kv_ref[slot_of(offset), 1, BLOCK:, :], weights.astype(jnp.bfloat16)
            )

    final = o_ref[...] / l_ref[...]
    for group in range(4):
        part = final[:, group * 128 : (group + 1) * 128]
        out_ref[:, group * 128 : (group + 1) * 128] = part.T.astype(jnp.bfloat16)


def attend(prefix_blocks, queries, own_keys, own_values, kv):
    vmem = pl.BlockSpec(memory_space=pltpu.VMEM)
    return pl.pallas_call(
        attend_kernel,
        out_shape=jax.ShapeDtypeStruct((128, 512), jnp.bfloat16),
        in_specs=[pl.BlockSpec(memory_space=pltpu.SMEM)] + [vmem] * 4,
        out_specs=vmem,
        scratch_shapes=[
            pltpu.VMEM((REACH + 1, BLOCK, 512), jnp.float32),
            pltpu.VMEM((1, 512), jnp.float32),
            pltpu.VMEM((1, 512), jnp.float32),
            pltpu.VMEM((HEAD_DIM, 512), jnp.float32),
        ],
        compiler_params=pltpu.CompilerParams(vmem_limit_bytes=24 * 1024 * 1024),
        name="attend",
    )(prefix_blocks, queries, own_keys, own_values, kv)


def on_device(slice_rows, w_query, w_key, w_value, prefix_keys, prefix_values, prefix_blocks):
    queries, own_keys, own_values, kv = gather(
        slice_rows, w_query, w_key, w_value, prefix_keys, prefix_values
    )
    return attend(prefix_blocks, queries, own_keys, own_values, kv)


def solution(mesh):
    in_specs = (
        P("section", "head"),
        P(None, "head"),
        P(None, "head"),
        P(None, "head"),
        P("section", "head"),
        P("section", "head"),
        P(),
    )
    out_specs = P("section", "head")
    return jax.shard_map(
        on_device, mesh=mesh, in_specs=in_specs, out_specs=out_specs, check_vma=False
    )
```

```python
import functools
import math

import jax
import jax.numpy as jnp
from jax import lax
from jax.experimental import pallas as pl
from jax.experimental.pallas import tpu as pltpu
from jax.sharding import PartitionSpec as P

HEAD_DIM = 128
BLOCK = 256
REACH = 7
COLUMNS = 4
LAYERS = 8
RING = 8
MESH = pl.DeviceIdType.MESH

LOW_FIRST = [0, 1, 2, 3]
HIGH_FIRST = [2, 3, 0, 1]
LOW, HIGH = (0, 1), (2, 3)
RELAY = 4
DEFERRED = 5.0
PIECES = 4
PIECE = 128 // PIECES


def rows_of(piece):
    return pl.ds((piece // 2) * BLOCK, BLOCK)


def steps(first, each=1.4):
    return [first + each * index for index in range(4)]


def arrivals(column):
    events = []

    def add(times, slot, order=LOW_FIRST, kinds=(0, 1), right=(), left=(), up=(), pair=True, prev=None):
        for time, piece in zip(times, order):
            events.append(
                dict(
                    time=time, slot=slot, kinds=kinds, piece=piece,
                    right=piece in right, left=piece in left, up=piece in up, pair=pair,
                    prev=slot >= column if prev is None else prev,
                )
            )

    every = LOW + HIGH
    direct, relayed = steps(4.2), steps(6.9)
    if column < 3:
        add(steps(4.0, 0.7), column, kinds=(1,))
        order = HIGH_FIRST if column == 2 else LOW_FIRST
        add(direct, RELAY, order, up=every, pair=False, prev=False)
    if column == 0:
        add(relayed, 1)
        add(steps(7.6), 3, right=LOW)
        add([9.3, 10.7], 2, LOW)
        add([10.8, 12.2], 2, HIGH)
    elif column == 1:
        add(direct, 0, right=LOW)
        add(relayed, 2, left=LOW)
        add([10.0, 11.4], 3, LOW)
        add([9.3, 10.7], 3, HIGH)
    elif column == 2:
        add(direct, 1, right=every)
        add(relayed, 3, HIGH_FIRST, left=HIGH)
        add([8.0, 9.4], 0, LOW)
        add([8.0, 9.4], 0, HIGH)
    else:
        add(steps(4.9), 3, right=every)
        add(direct, 2, HIGH_FIRST, up=HIGH)
        add(direct, 0, HIGH_FIRST, left=HIGH)
        add([8.4, 9.8], RELAY, HIGH, right=HIGH, pair=False, prev=True)
        add(steps(8.3), 1)
    return sorted(events, key=lambda event: event["time"])


def gather_kernel(
    x_ref, wq_ref, wk_ref, wv_ref, pk_ref, pv_ref,
    q_ref, k_ref, v_ref, kv_ref,
    xbuf, xother, weights, acc, relay,
    w_sem, local_sem, x_send, x_recv, x_pair_send, x_pair_recv,
    right_send, left_send, up_send, own_send, relay_send, right_fwd, left_fwd, pair_send,
    slot_recv, relay_recv, pair_recv, ready,
):
    section = lax.axis_index("section")
    y = lax.axis_index("head")
    core = lax.rem(section, 2)
    x = lax.rem(lax.div(section, 2), COLUMNS)
    z = lax.div(section, 2 * COLUMNS)

    def at(layer, column, kind, ring=None):
        return ((layer * COLUMNS + column) * 2 + kind, y if ring is None else ring)

    x_right, x_left = lax.rem(x + 1, COLUMNS), lax.rem(x + COLUMNS - 1, COLUMNS)
    z_above, z_below = lax.rem(z + 1, LAYERS), lax.rem(z + LAYERS - 1, LAYERS)
    y_up, y_down = lax.rem(y + 1, RING), lax.rem(y + RING - 1, RING)
    right, left = at(z, x_right, 1), at(z, x_left, 1)
    above = at(z_above, x, 1)
    ways = (at(z, x, 1, y_up), at(z, x, 1, y_down))
    pair = at(z, x, 1 - core)

    def block_at(hop):
        return lax.rem(y + hop + RING, RING)

    visits = [0, -1, 1, -2, 2, -3, 3, 4]

    def start_weights(hop):
        start = pl.multiple_of(block_at(hop) * 512, 512)
        rows = pl.ds(start, 512)
        for source, first, size in ((wq_ref, 0, 512), (wk_ref, 512, 128), (wv_ref, 640, 128)):
            pltpu.make_async_copy(
                source.at[rows], weights.at[rows, first : first + size], w_sem.at[min(abs(hop), 1)]
            ).start()

    def wait_weights(index, blocks):
        rows = weights.at[: blocks * 512]
        pltpu.make_async_copy(rows, rows, w_sem.at[index]).wait()

    def project(hop):
        start = pl.multiple_of(block_at(hop) * 512, 512)
        part = jnp.dot(
            xbuf[block_at(hop)], weights[pl.ds(start, 512), :], preferred_element_type=jnp.float32
        )
        if hop == 0:
            acc[...] = part
        else:
            acc[...] += part

    def remote(source, target, send, recv, device):
        return pltpu.make_async_remote_copy(
            src_ref=source, dst_ref=target, send_sem=send, recv_sem=recv,
            device_id=device, device_id_type=MESH,
        )

    own_x = pltpu.make_async_copy(x_ref, xbuf.at[y], local_sem.at[0])
    own_x.start()
    start_weights(0)

    def tell(semaphore, device):
        pl.semaphore_signal(semaphore, inc=1, device_id=device, device_id_type=MESH)

    barrier = pltpu.get_barrier_semaphore()

    @pl.when(core == 1)
    def _():
        for kind in range(2):
            for device in (
                at(z, x, kind, y_up), at(z, x, kind, y_down),
                at(z, x_right, kind), at(z, x_left, kind),
            ):
                tell(barrier, device)

    tell(barrier, pair)

    @pl.when((z < LAYERS - 1) & ((core == 1) | (x == 3)))
    def _():
        tell(barrier, above)

    for hop in visits[1:]:
        start_weights(hop)
    pltpu.make_async_copy(pk_ref, kv_ref.at[8, 0], local_sem.at[1]).start()
    pltpu.make_async_copy(pv_ref, kv_ref.at[8, 1], local_sem.at[1]).start()
    below_count = jnp.where((core == 1) & (z > 0), jnp.where(x == 3, 2, 1), 0)
    pl.semaphore_wait(barrier, 5 + below_count)

    @pl.when((core == 1) & (z > 0))
    def _():
        tell(ready, at(z_below, x, 1))

        @pl.when(x == 3)
        def _():
            tell(ready, at(z_below, x, 0))

    def received(here, semaphore):
        remote(here, here, own_send, semaphore, pair).wait_recv()

    def sent(here, semaphore):
        remote(here, here, semaphore, pair_recv, pair).wait_send()

    def pieces_of(count):
        return kv_ref.at[0, 0, : 256 * count] if count < 3 else kv_ref.at[: count // 4]

    def rows_at(piece):
        return pl.ds(piece * PIECE, PIECE)

    def x_own(way, piece, kind):
        target = xother if kind == 0 else xbuf
        return remote(
            x_ref.at[rows_at(piece)], target.at[y, rows_at(piece)],
            x_send.at[way], x_recv.at[way, piece], ways[way],
        )

    def x_origin(way, hop):
        return block_at(-hop - 1 if way == 0 else hop + 1)

    def x_piece(way, hop, piece, kind):
        return (xother if kind == 0 else xbuf).at[x_origin(way, hop), rows_at(piece)]

    def x_forward(way, hop, piece, kind):
        here = x_piece(way, hop, piece, kind)
        index = (hop + 1) * PIECES + piece
        return remote(here, here, x_send.at[way], x_recv.at[way, index], ways[way])

    def x_hand(way, hop, piece):
        rows = rows_at(piece)
        return remote(
            xother.at[x_origin(way, hop), rows], xbuf.at[x_origin(way, hop), rows],
            x_pair_send, x_pair_recv.at[min(hop * 2 + way, 6)], pair,
        )

    def travels(way, hop, piece):
        return hop < 3 or (hop == 3 and piece // (PIECES // 2) == way)

    def own_piece(piece):
        return (pk_ref if piece % 2 == 0 else pv_ref).at[rows_of(piece)]

    def slot_piece(column, kind, piece):
        return kv_ref.at[column * 2 + kind, piece % 2, rows_of(piece)]

    def relay_piece(kind, piece):
        return relay.at[kind, piece % 2, rows_of(piece)]

    def send_right(kind, piece, column):
        return remote(
            own_piece(piece), slot_piece(column, kind, piece),
            right_send, slot_recv.at[column, piece], right,
        )

    def send_left(kind, piece, column):
        if column == 0:
            target, arrived = slot_piece(0, kind, piece), slot_recv.at[0, piece]
        else:
            target, arrived = relay_piece(kind, piece), relay_recv.at[piece]
        return remote(own_piece(piece), target, left_send, arrived, left)

    def send_up(kind, piece):
        if kind == 0:
            target, arrived = relay_piece(2, piece), slot_recv.at[x, piece]
        else:
            target, arrived = slot_piece(x, 1, piece), slot_recv.at[x, piece]
        return remote(own_piece(piece), target, up_send, arrived, above)

    def send_pair(piece):
        return remote(
            own_piece(piece), slot_piece(x, 0, piece),
            own_send, pair_recv, pair,
        )

    def first_sends(kind, column):
        leftward = HIGH_FIRST if column in (0, 3) else LOW_FIRST
        rightward = HIGH_FIRST if column == 2 else LOW_FIRST
        for index in range(4):
            yield column > 0, functools.partial(send_left, kind, leftward[index], column)
            if column < 3:
                yield False, functools.partial(send_right, kind, rightward[index], column)

    def source_of(event, column, kind):
        if event["slot"] == RELAY:
            return relay_piece(kind, event["piece"])
        if column == 3 and event["slot"] == 3 and kind == 0:
            return relay_piece(2, event["piece"])
        return slot_piece(event["slot"], kind, event["piece"])

    def sends_of(event, column, upward):
        for kind in event["kinds"]:
            piece, slot = event["piece"], event["slot"]
            source = source_of(event, column, kind)
            if upward:
                if event["up"] and column < 3:
                    yield remote(
                        source, slot_piece(column + 1, kind, piece), relay_send,
                        slot_recv.at[column + 1, piece], above,
                    )
                elif event["up"]:
                    yield remote(
                        source, relay_piece(kind, piece), relay_send, relay_recv.at[piece], above
                    )
                continue
            if slot == RELAY:
                slot = 2
            target, arrived = slot_piece(slot, kind, piece), slot_recv.at[slot, piece]
            if event["right"]:
                yield remote(source, target, right_fwd, arrived, right)
            if event["left"]:
                yield remote(source, target, left_fwd, arrived, left)
            if event["pair"] and (slot != column or kind == 1):
                yield remote(source, target, pair_send, pair_recv, pair)

    def count(column, what, prevs):
        total = 0
        for event in arrivals(column):
            if event[what] and (prevs or not event["prev"]):
                kinds = (1,) if what == "pair" and event["slot"] == column else event["kinds"]
                total += len(kinds)
        return total

    def guarded(condition, run):
        if condition is None:
            run()
        else:
            pl.when(condition)(run)

    def start_first(kind):
        for piece in range(PIECES):
            for way in range(2):
                x_own(way, piece, kind).start()
        for column in range(COLUMNS):

            @pl.when(x == column)
            def _():
                plain = [make for needs, make in first_sends(kind, column) if not needs]
                needing = [make for needs, make in first_sends(kind, column) if needs]
                if needing:

                    @pl.when(z < LAYERS - 1)
                    def _():
                        for make in needing:
                            make().start()

                for make in plain:
                    make().start()

    def finish_first(kind):
        @pl.when((x == 0) | (z < LAYERS - 1))
        def _():
            sent(pieces_of(4), left_send)

        @pl.when(x < 3)
        def _():
            sent(pieces_of(4), right_send)

        @pl.when((z < LAYERS - 1) & (x == 3) if kind == 0 else z < LAYERS - 1)
        def _():
            sent(pieces_of(4), up_send)

    @pl.when(z == 0)
    def _():
        for column in range(COLUMNS):

            @pl.when(x == column)
            def _():
                for slot in range(column * 2 + 2, COLUMNS * 2):
                    kv_ref[slot] = jnp.zeros((2, 512, HEAD_DIM), jnp.bfloat16)

                @pl.when(core == 0)
                def _():
                    kv_ref[column * 2 + 1] = jnp.zeros((2, 512, HEAD_DIM), jnp.bfloat16)

    @pl.when(core == 0)
    def _():
        start_first(0)
        for piece in range(4):
            send_pair(piece).start()
        own_x.wait()
        wait_weights(0, 1)
        project(0)

        @pl.when((x == 3) & (z < LAYERS - 1))
        def _():
            pl.semaphore_wait(ready, 1)
            for piece in range(4):
                send_up(0, piece).start()

        wait_weights(1, 7)
        for index, hop in enumerate(visits[1:]):
            received(xbuf.at[0], x_pair_recv.at[index])
            project(hop)

        @pl.when(z > 0)
        def _():
            received(pieces_of(28), pair_recv)

        for column in range(1, COLUMNS):

            @pl.when((z == 0) & (x == column))
            def _():
                received(pieces_of(8 * column), pair_recv)

        finish_first(0)
        sent(pieces_of(4), own_send)
        for way in range(2):
            sent(xbuf.at[0], x_send.at[way])

    schedules = [arrivals(column) for column in range(COLUMNS)]

    def handle(event, column):
        def run():
            semaphore = (relay_recv if event["slot"] == RELAY else slot_recv.at[event["slot"]]).at[event["piece"]]
            received(pieces_of(len(event["kinds"])), semaphore)
            if event["up"]:
                held = event["time"] <= DEFERRED

                @pl.when((z > 0) & (z < LAYERS - 1) if held else z < LAYERS - 1)
                def _():
                    for copy in sends_of(event, column, True):
                        copy.start()

            for copy in sends_of(event, column, False):
                copy.start()

        whole = event["slot"] == RELAY and event["up"]
        guarded(z < LAYERS - 1 if whole else z > 0 if event["prev"] else None, run)

    def prefixes(until):
        for column in range(COLUMNS):
            due = [event for event in schedules[column] if event["time"] <= until]
            if not due:
                continue
            schedules[column] = schedules[column][len(due) :]

            @pl.when(x == column)
            def _():
                for event in due:
                    handle(event, column)

    def lowest_goes_up():
        @pl.when(z == 0)
        def _():
            pl.semaphore_wait(ready, 1)
            for piece in range(4):
                send_up(1, piece).start()
            for column in range(COLUMNS):

                @pl.when(x == column)
                def _():
                    for event in arrivals(column):
                        if event["up"] and event["time"] <= DEFERRED:
                            for copy in sends_of(event, column, True):
                                copy.start()

    @pl.when(core == 1)
    def _():
        start_first(1)

        @pl.when((z > 0) & (z < LAYERS - 1))
        def _():
            pl.semaphore_wait(ready, 1)
            for piece in range(4):
                send_up(1, piece).start()

        own_x.wait()
        wait_weights(0, 1)
        project(0)
        clock = {0: 3.5, 1: 5.9, 2: 8.3, 3: 10.7}
        for hop in range(4):
            for piece in range(PIECES):
                if hop == 3 and piece >= PIECES // 2:
                    continue
                for way in range(2):
                    this = piece if hop < 3 or way == 0 else piece + PIECES // 2
                    received(xbuf.at[0, : 2 * PIECE], x_recv.at[way, hop * PIECES + this])
                    for kind in range(2):
                        if travels(way, hop + 1, this):
                            x_forward(way, hop, this, kind).start()
                    x_hand(way, hop, this).start()
                prefixes(clock[hop] + 2.4 / PIECES * piece)
                if hop == 0 and piece == PIECES - 1:
                    lowest_goes_up()
                    wait_weights(1, 7)
                if hop > 0 and piece == 0:
                    project(-hop)
                if hop > 0 and piece == 1:
                    project(hop)
        project(4)
        prefixes(99.0)
        received(pieces_of(4), pair_recv)

        finish_first(1)
        for way in range(2):
            sent(xbuf.at[:6], x_send.at[way])
        sent(xbuf.at[:7], x_pair_send)
        for column in range(COLUMNS):

            @pl.when(x == column)
            def _():
                for condition, prevs in ((z > 0, True), (z == 0, False)):

                    @pl.when(condition)
                    def _():
                        for what, semaphore in (("pair", pair_send), ("right", right_fwd), ("left", left_fwd)):
                            total = count(column, what, prevs)
                            if total:
                                sent(pieces_of(total), semaphore)

                @pl.when(z < LAYERS - 1)
                def _():
                    sent(pieces_of(count(column, "up", True)), relay_send)

    for group in range(4):
        q_ref[group * 128 : (group + 1) * 128, :] = acc[:, group * 128 : (group + 1) * 128].astype(jnp.bfloat16)
    k_ref[...] = acc[:, 512:640].astype(jnp.bfloat16)
    v_ref[...] = acc[:, 640:768].astype(jnp.bfloat16)
    pltpu.make_async_copy(kv_ref.at[8], kv_ref.at[8], local_sem.at[1]).wait()


def gather(slice_rows, w_query, w_key, w_value, prefix_keys, prefix_values):
    bf16, f32 = jnp.bfloat16, jnp.float32
    dma = pltpu.SemaphoreType.DMA
    anywhere = pl.BlockSpec(memory_space=pltpu.HBM)
    vmem = pl.BlockSpec(memory_space=pltpu.VMEM)
    return pl.pallas_call(
        gather_kernel,
        out_shape=(
            pltpu.VMEM((512, HEAD_DIM), bf16),
            pltpu.VMEM((128, HEAD_DIM), bf16),
            pltpu.VMEM((128, HEAD_DIM), bf16),
            pltpu.VMEM((9, 2, 512, HEAD_DIM), bf16),
        ),
        in_specs=[anywhere] * 6,
        out_specs=(vmem,) * 4,
        scratch_shapes=[
            pltpu.VMEM((RING, 128, 512), bf16),
            pltpu.VMEM((RING, 128, 512), bf16),
            pltpu.VMEM((4096, 768), bf16),
            pltpu.VMEM((128, 768), f32),
            pltpu.VMEM((3, 2, 512, HEAD_DIM), bf16),
            dma((2,)), dma((2,)),
            dma((2,)), dma((2, 4 * PIECES)), dma, dma((7,)),
            dma, dma, dma, dma, dma, dma, dma, dma,
            dma((4, 4)), dma((4,)), dma, pltpu.SemaphoreType.REGULAR,
        ],
        compiler_params=pltpu.CompilerParams(
            collective_id=0, has_side_effects=True, vmem_limit_bytes=58 * 1024 * 1024
        ),
        name="gather",
    )(slice_rows, w_query, w_key, w_value, prefix_keys, prefix_values)


def scores_of(keys, queries):
    return lax.dot_general(
        keys, queries, (((1,), (1,)), ((), ())), preferred_element_type=jnp.float32
    )


def weigh(values, weights):
    return lax.dot_general(
        values, weights, (((0,), (0,)), ((), ())), preferred_element_type=jnp.float32
    )


def attend_kernel(pb_ref, q_ref, k_ref, v_ref, kv_ref, out_ref, scores, m_ref, l_ref, o_ref):
    section = lax.axis_index("section")
    factor = math.log2(math.e) / math.sqrt(HEAD_DIM)
    never = 1e30
    queries = q_ref[...]

    def slot_of(offset):
        return 8 if offset == 0 else lax.rem(section - offset + 64, 8)

    key_row = lax.broadcasted_iota(jnp.int32, (128, 512), 0)
    query_row = lax.broadcasted_iota(jnp.int32, (128, 512), 1) % 128
    own = jnp.where(key_row <= query_row, scores_of(k_ref[...], queries), -never)
    top = jnp.max(own, axis=0, keepdims=True)
    for offset in range(REACH + 1):
        part = scores_of(kv_ref[slot_of(offset), 0, :BLOCK, :], queries)
        scores[offset] = part
        peak = jnp.max(part, axis=0, keepdims=True)
        top = jnp.maximum(top, jnp.where(section >= offset, peak, -never))
    weights = jnp.exp2((own - top) * factor)
    total = jnp.sum(weights, axis=0, keepdims=True)
    result = weigh(v_ref[...], weights.astype(jnp.bfloat16))
    for offset in range(REACH + 1):
        shift = jnp.where(section >= offset, top, never)
        weights = jnp.exp2((scores[offset] - shift) * factor)
        total += jnp.sum(weights, axis=0, keepdims=True)
        result += weigh(kv_ref[slot_of(offset), 1, :BLOCK, :], weights.astype(jnp.bfloat16))
    m_ref[...] = top
    l_ref[...] = total
    o_ref[...] = result

    for offset in range(REACH + 1):
        blocks = pb_ref[jnp.maximum(section - offset, 0)]

        @pl.when((section >= offset) & (blocks > 1))
        def _():
            part = scores_of(kv_ref[slot_of(offset), 0, BLOCK:, :], queries)
            before = m_ref[...]
            after = jnp.maximum(before, jnp.max(part, axis=0, keepdims=True))
            keep = jnp.exp2((before - after) * factor)
            weights = jnp.exp2((part - after) * factor)
            m_ref[...] = after
            l_ref[...] = l_ref[...] * keep + jnp.sum(weights, axis=0, keepdims=True)
            o_ref[...] = o_ref[...] * keep + weigh(
                kv_ref[slot_of(offset), 1, BLOCK:, :], weights.astype(jnp.bfloat16)
            )

    final = o_ref[...] / l_ref[...]
    for group in range(4):
        part = final[:, group * 128 : (group + 1) * 128]
        out_ref[:, group * 128 : (group + 1) * 128] = part.T.astype(jnp.bfloat16)


def attend(prefix_blocks, queries, own_keys, own_values, kv):
    vmem = pl.BlockSpec(memory_space=pltpu.VMEM)
    return pl.pallas_call(
        attend_kernel,
        out_shape=jax.ShapeDtypeStruct((128, 512), jnp.bfloat16),
        in_specs=[pl.BlockSpec(memory_space=pltpu.SMEM)] + [vmem] * 4,
        out_specs=vmem,
        scratch_shapes=[
            pltpu.VMEM((REACH + 1, BLOCK, 512), jnp.float32),
            pltpu.VMEM((1, 512), jnp.float32),
            pltpu.VMEM((1, 512), jnp.float32),
            pltpu.VMEM((HEAD_DIM, 512), jnp.float32),
        ],
        compiler_params=pltpu.CompilerParams(vmem_limit_bytes=24 * 1024 * 1024),
        name="attend",
    )(prefix_blocks, queries, own_keys, own_values, kv)


def on_device(slice_rows, w_query, w_key, w_value, prefix_keys, prefix_values, prefix_blocks):
    queries, own_keys, own_values, kv = gather(
        slice_rows, w_query, w_key, w_value, prefix_keys, prefix_values
    )
    return attend(prefix_blocks, queries, own_keys, own_values, kv)


def solution(mesh):
    in_specs = (
        P("section", "head"),
        P(None, "head"),
        P(None, "head"),
        P(None, "head"),
        P("section", "head"),
        P("section", "head"),
        P(),
    )
    out_specs = P("section", "head")
    return jax.shard_map(
        on_device, mesh=mesh, in_specs=in_specs, out_specs=out_specs, check_vma=False
    )
```

```python
import functools
import math

import jax
import jax.numpy as jnp
from jax import lax
from jax.experimental import pallas as pl
from jax.experimental.pallas import tpu as pltpu
from jax.sharding import PartitionSpec as P

HEAD_DIM = 128
BLOCK = 256
REACH = 7
COLUMNS = 4
LAYERS = 8
RING = 8
MESH = pl.DeviceIdType.MESH

SPLIT = 8
ROWS = 2 * 512 // SPLIT
LOW, HIGH = tuple(range(SPLIT // 2)), tuple(range(SPLIT // 2, SPLIT))
LOW_FIRST, HIGH_FIRST = LOW + HIGH, HIGH + LOW
RELAY = 4
PIECES = 8
PIECE = 128 // PIECES


def clock(hop, piece):
    return 3.5 + 2.4 * hop + 2.4 / PIECES * piece


DEFERRED = clock(0, PIECES - 1)


def rows_of(piece):
    return pl.ds((piece // 2) * ROWS, ROWS)


def steps(first, each=5.6 / SPLIT):
    return [first + each * index for index in range(SPLIT)]


def arrivals(column):
    events = []

    def add(times, slot, order=LOW_FIRST, kinds=(0, 1), right=(), left=(), up=(), pair=True, prev=None):
        for time, piece in zip(times, order):
            events.append(
                dict(
                    time=time, slot=slot, kinds=kinds, piece=piece,
                    right=piece in right, left=piece in left, up=piece in up, pair=pair,
                    prev=slot >= column if prev is None else prev,
                )
            )

    every = LOW + HIGH
    direct, relayed = steps(3.5), steps(6.5)
    if column < 3:
        add(steps(7.0, 2.8 / SPLIT), column, kinds=(1,))
        order = HIGH_FIRST if column == 2 else LOW_FIRST
        add(direct, RELAY, order, up=every, pair=False, prev=False)
    if column == 0:
        add(relayed, 1)
        add(steps(7.1), 3, right=LOW)
        add(steps(8.3), 2)
    elif column == 1:
        add(direct, 0, right=LOW)
        add(relayed, 2, left=every)
        add(steps(9.5), 3, LOW)
        add(steps(8.3), 3, HIGH)
    elif column == 2:
        add(direct, 1, right=every)
        add(relayed, 3, HIGH_FIRST, left=HIGH)
        add(steps(8.0), 0, LOW)
        add(steps(8.0), 0, HIGH)
    else:
        add(steps(4.2), 3, right=every)
        add(direct, 2)
        add(direct, 0, HIGH_FIRST, left=HIGH)
        add(steps(8.0), 1)
    return sorted(events, key=lambda event: event["time"])


def gather_kernel(
    x_ref, wq_ref, wk_ref, wv_ref, pk_ref, pv_ref,
    q_ref, k_ref, v_ref, kv_ref,
    xbuf, xother, weights, acc, relay,
    w_sem, local_sem, x_send, x_recv, x_pair_send, x_pair_recv,
    right_send, left_send, up_send, own_send, relay_send, right_fwd, left_fwd, pair_send,
    slot_recv, relay_recv, pair_recv, ready,
):
    section = lax.axis_index("section")
    y = lax.axis_index("head")
    core = lax.rem(section, 2)
    x = lax.rem(lax.div(section, 2), COLUMNS)
    z = lax.div(section, 2 * COLUMNS)

    def at(layer, column, kind, ring=None):
        return ((layer * COLUMNS + column) * 2 + kind, y if ring is None else ring)

    x_right, x_left = lax.rem(x + 1, COLUMNS), lax.rem(x + COLUMNS - 1, COLUMNS)
    z_above, z_below = lax.rem(z + 1, LAYERS), lax.rem(z + LAYERS - 1, LAYERS)
    y_up, y_down = lax.rem(y + 1, RING), lax.rem(y + RING - 1, RING)
    right, left = at(z, x_right, 1), at(z, x_left, 1)
    above = at(z_above, x, 1)
    ways = (at(z, x, 1, y_up), at(z, x, 1, y_down))
    pair = at(z, x, 1 - core)

    def block_at(hop):
        return lax.rem(y + hop + RING, RING)

    visits = [0, -1, 1, -2, 2, -3, 3, 4]

    def start_weights(hop):
        start = pl.multiple_of(block_at(hop) * 512, 512)
        rows = pl.ds(start, 512)
        for source, first, size in ((wq_ref, 0, 512), (wk_ref, 512, 128), (wv_ref, 640, 128)):
            pltpu.make_async_copy(
                source.at[rows], weights.at[rows, first : first + size], w_sem.at[min(abs(hop), 1)]
            ).start()

    def wait_weights(index, blocks):
        rows = weights.at[: blocks * 512]
        pltpu.make_async_copy(rows, rows, w_sem.at[index]).wait()

    def project(hop):
        start = pl.multiple_of(block_at(hop) * 512, 512)
        part = jnp.dot(
            xbuf[block_at(hop)], weights[pl.ds(start, 512), :], preferred_element_type=jnp.float32
        )
        if hop == 0:
            acc[...] = part
        else:
            acc[...] += part

    def remote(source, target, send, recv, device):
        return pltpu.make_async_remote_copy(
            src_ref=source, dst_ref=target, send_sem=send, recv_sem=recv,
            device_id=device, device_id_type=MESH,
        )

    own_x = pltpu.make_async_copy(x_ref, xbuf.at[y], local_sem.at[0])
    own_x.start()
    start_weights(0)

    def tell(semaphore, device):
        pl.semaphore_signal(semaphore, inc=1, device_id=device, device_id_type=MESH)

    barrier = pltpu.get_barrier_semaphore()

    @pl.when(core == 1)
    def _():
        for kind in range(2):
            for device in (
                at(z, x, kind, y_up), at(z, x, kind, y_down),
                at(z, x_right, kind), at(z, x_left, kind),
            ):
                tell(barrier, device)

    tell(barrier, pair)

    @pl.when((z < LAYERS - 1) & ((core == 1) | (x == 3)))
    def _():
        tell(barrier, above)

    for hop in visits[1:]:
        start_weights(hop)
    pltpu.make_async_copy(pk_ref, kv_ref.at[8, 0], local_sem.at[1]).start()
    pltpu.make_async_copy(pv_ref, kv_ref.at[8, 1], local_sem.at[1]).start()
    below_count = jnp.where((core == 1) & (z > 0), jnp.where(x == 3, 2, 1), 0)
    pl.semaphore_wait(barrier, 5 + below_count)

    @pl.when((core == 1) & (z > 0))
    def _():
        tell(ready, at(z_below, x, 1))

        @pl.when(x == 3)
        def _():
            tell(ready, at(z_below, x, 0))

    def received(here, semaphore):
        remote(here, here, own_send, semaphore, pair).wait_recv()

    def sent(here, semaphore):
        remote(here, here, semaphore, pair_recv, pair).wait_send()

    def pieces_of(count):
        return kv_ref.at[0, 0, : ROWS * count] if count < 3 else kv_ref.at[: count // SPLIT]

    def rows_at(piece):
        return pl.ds(piece * PIECE, PIECE)

    def x_own(way, piece, kind):
        target = xother if kind == 0 else xbuf
        return remote(
            x_ref.at[rows_at(piece)], target.at[y, rows_at(piece)],
            x_send.at[way], x_recv.at[way, piece], ways[way],
        )

    def x_origin(way, hop):
        return block_at(-hop - 1 if way == 0 else hop + 1)

    def x_piece(way, hop, piece, kind):
        return (xother if kind == 0 else xbuf).at[x_origin(way, hop), rows_at(piece)]

    def x_forward(way, hop, piece, kind):
        here = x_piece(way, hop, piece, kind)
        index = (hop + 1) * PIECES + piece
        return remote(here, here, x_send.at[way], x_recv.at[way, index], ways[way])

    def x_hand(way, hop, piece):
        rows = rows_at(piece)
        return remote(
            xother.at[x_origin(way, hop), rows], xbuf.at[x_origin(way, hop), rows],
            x_pair_send, x_pair_recv.at[min(hop * 2 + way, 6)], pair,
        )

    def travels(way, hop, piece):
        return hop < 3 or (hop == 3 and piece // (PIECES // 2) == way)

    def own_piece(piece):
        return (pk_ref if piece % 2 == 0 else pv_ref).at[rows_of(piece)]

    def slot_piece(column, kind, piece):
        return kv_ref.at[column * 2 + kind, piece % 2, rows_of(piece)]

    def relay_piece(kind, piece):
        return relay.at[kind, piece % 2, rows_of(piece)]

    def send_right(kind, piece, column):
        return remote(
            own_piece(piece), slot_piece(column, kind, piece),
            right_send, slot_recv.at[column, piece], right,
        )

    def send_left(kind, piece, column):
        if column == 0:
            target, arrived = slot_piece(0, kind, piece), slot_recv.at[0, piece]
        else:
            target, arrived = relay_piece(kind, piece), relay_recv.at[piece]
        return remote(own_piece(piece), target, left_send, arrived, left)

    def send_up(kind, piece):
        if kind == 0:
            target, arrived = relay_piece(2, piece), slot_recv.at[x, piece]
        else:
            target, arrived = slot_piece(x, 1, piece), slot_recv.at[x, piece]
        return remote(own_piece(piece), target, up_send, arrived, above)

    def send_pair(piece):
        return remote(
            own_piece(piece), slot_piece(x, 0, piece),
            own_send, pair_recv, pair,
        )

    def first_sends(kind, column):
        leftward = HIGH_FIRST if column in (0, 3) else LOW_FIRST
        for index in range(SPLIT):
            yield column > 0, functools.partial(send_left, kind, leftward[index], column)
            if column < 3:
                yield False, functools.partial(send_right, kind, index, column)

    def source_of(event, column, kind):
        if event["slot"] == RELAY:
            return relay_piece(kind, event["piece"])
        if column == 3 and event["slot"] == 3 and kind == 0:
            return relay_piece(2, event["piece"])
        return slot_piece(event["slot"], kind, event["piece"])

    def sends_of(event, column, upward):
        for kind in event["kinds"]:
            piece, slot = event["piece"], event["slot"]
            source = source_of(event, column, kind)
            if upward:
                if event["up"]:
                    yield remote(
                        source, slot_piece(column + 1, kind, piece), relay_send,
                        slot_recv.at[column + 1, piece], above,
                    )
                continue
            if slot == RELAY:
                continue
            target, arrived = slot_piece(slot, kind, piece), slot_recv.at[slot, piece]
            if event["right"]:
                yield remote(source, target, right_fwd, arrived, right)
            if event["left"]:
                yield remote(source, target, left_fwd, arrived, left)
            if event["pair"] and (slot != column or kind == 1):
                yield remote(source, target, pair_send, pair_recv, pair)

    def count(column, what, prevs):
        total = 0
        for event in arrivals(column):
            if event[what] and (prevs or not event["prev"]):
                kinds = (1,) if what == "pair" and event["slot"] == column else event["kinds"]
                total += len(kinds)
        return total

    def guarded(condition, run):
        if condition is None:
            run()
        else:
            pl.when(condition)(run)

    def start_first(kind):
        for piece in range(PIECES):
            for way in range(2):
                x_own(way, piece, kind).start()
        for column in range(COLUMNS):

            @pl.when(x == column)
            def _():
                plain = [make for needs, make in first_sends(kind, column) if not needs]
                needing = [make for needs, make in first_sends(kind, column) if needs]
                if needing:

                    @pl.when(z < LAYERS - 1)
                    def _():
                        for make in needing:
                            make().start()

                for make in plain:
                    make().start()

    def finish_first(kind):
        @pl.when((x == 0) | (z < LAYERS - 1))
        def _():
            sent(pieces_of(SPLIT), left_send)

        @pl.when(x < 3)
        def _():
            sent(pieces_of(SPLIT), right_send)

        @pl.when((z < LAYERS - 1) & (x == 3) if kind == 0 else z < LAYERS - 1)
        def _():
            sent(pieces_of(SPLIT), up_send)

    @pl.when(z == 0)
    def _():
        for column in range(COLUMNS):

            @pl.when(x == column)
            def _():
                for slot in range(column * 2 + 2, COLUMNS * 2):
                    kv_ref[slot] = jnp.zeros((2, 512, HEAD_DIM), jnp.bfloat16)

                @pl.when(core == 0)
                def _():
                    kv_ref[column * 2 + 1] = jnp.zeros((2, 512, HEAD_DIM), jnp.bfloat16)

    @pl.when(core == 0)
    def _():
        start_first(0)
        for piece in range(SPLIT):
            send_pair(piece).start()
        own_x.wait()
        wait_weights(0, 1)
        project(0)

        @pl.when((x == 3) & (z < LAYERS - 1))
        def _():
            pl.semaphore_wait(ready, 1)
            for piece in range(SPLIT):
                send_up(0, piece).start()

        wait_weights(1, 7)
        for index, hop in enumerate(visits[1:]):
            received(xbuf.at[0], x_pair_recv.at[index])
            project(hop)

        @pl.when(z > 0)
        def _():
            received(pieces_of(7 * SPLIT), pair_recv)

        for column in range(1, COLUMNS):

            @pl.when((z == 0) & (x == column))
            def _():
                received(pieces_of(2 * SPLIT * column), pair_recv)

        finish_first(0)
        sent(pieces_of(SPLIT), own_send)
        for way in range(2):
            sent(xbuf.at[0], x_send.at[way])

    schedules = [arrivals(column) for column in range(COLUMNS)]

    def handle(event, column):
        def run():
            semaphore = (relay_recv if event["slot"] == RELAY else slot_recv.at[event["slot"]]).at[event["piece"]]
            received(pieces_of(len(event["kinds"])), semaphore)
            if event["up"]:
                held = event["time"] <= DEFERRED

                @pl.when((z > 0) & (z < LAYERS - 1) if held else z < LAYERS - 1)
                def _():
                    for copy in sends_of(event, column, True):
                        copy.start()

            for copy in sends_of(event, column, False):
                copy.start()

        whole = event["slot"] == RELAY and event["up"]
        guarded((z > 0) & (z < LAYERS - 1) if whole and column == 0 else z < LAYERS - 1 if whole else z > 0 if event["prev"] else None, run)

    def prefixes(until):
        for column in range(COLUMNS):
            due = [event for event in schedules[column] if event["time"] <= until]
            if not due:
                continue
            schedules[column] = schedules[column][len(due) :]

            @pl.when(x == column)
            def _():
                for event in due:
                    handle(event, column)

    def lowest_goes_up():
        @pl.when(z == 0)
        def _():
            pl.semaphore_wait(ready, 1)
            for piece in range(SPLIT):
                send_up(1, piece).start()

            @pl.when(x == 0)
            def _():
                for event in arrivals(0):
                    if event["up"]:
                        received(pieces_of(2), relay_recv.at[event["piece"]])
                        for copy in sends_of(event, 0, True):
                            copy.start()

    def lowest_relays():
        for column in range(1, COLUMNS - 1):

            @pl.when((z == 0) & (x == column))
            def _():
                for event in arrivals(column):
                    if event["up"] and event["time"] <= DEFERRED:
                        for copy in sends_of(event, column, True):
                            copy.start()

    @pl.when(core == 1)
    def _():
        start_first(1)

        @pl.when((z > 0) & (z < LAYERS - 1))
        def _():
            pl.semaphore_wait(ready, 1)
            for piece in range(SPLIT):
                send_up(1, piece).start()

        own_x.wait()
        wait_weights(0, 1)
        project(0)
        lowest_goes_up()
        for hop in range(4):
            for piece in range(PIECES):
                if hop == 3 and piece >= PIECES // 2:
                    continue
                for way in range(2):
                    this = piece if hop < 3 or way == 0 else piece + PIECES // 2
                    received(xbuf.at[0, : 2 * PIECE], x_recv.at[way, hop * PIECES + this])
                    for kind in range(2):
                        if travels(way, hop + 1, this):
                            x_forward(way, hop, this, kind).start()
                    x_hand(way, hop, this).start()
                prefixes(clock(hop, piece))
                if hop == 0 and piece == PIECES - 1:
                    lowest_relays()
                    wait_weights(1, 7)
                if hop > 0 and piece == 0:
                    project(-hop)
                if hop > 0 and piece == 1:
                    project(hop)
        project(4)
        prefixes(99.0)
        received(pieces_of(SPLIT), pair_recv)

        finish_first(1)
        for way in range(2):
            sent(xbuf.at[:6], x_send.at[way])
        sent(xbuf.at[:7], x_pair_send)
        for column in range(COLUMNS):

            @pl.when(x == column)
            def _():
                for condition, prevs in ((z > 0, True), (z == 0, False)):

                    @pl.when(condition)
                    def _():
                        for what, semaphore in (("pair", pair_send), ("right", right_fwd), ("left", left_fwd)):
                            total = count(column, what, prevs)
                            if total:
                                sent(pieces_of(total), semaphore)

                if column < 3:

                    @pl.when(z < LAYERS - 1)
                    def _():
                        sent(pieces_of(2 * SPLIT), relay_send)

    for group in range(4):
        q_ref[group * 128 : (group + 1) * 128, :] = acc[:, group * 128 : (group + 1) * 128].astype(jnp.bfloat16)
    k_ref[...] = acc[:, 512:640].astype(jnp.bfloat16)
    v_ref[...] = acc[:, 640:768].astype(jnp.bfloat16)
    pltpu.make_async_copy(kv_ref.at[8], kv_ref.at[8], local_sem.at[1]).wait()


def gather(slice_rows, w_query, w_key, w_value, prefix_keys, prefix_values):
    bf16, f32 = jnp.bfloat16, jnp.float32
    dma = pltpu.SemaphoreType.DMA
    anywhere = pl.BlockSpec(memory_space=pltpu.HBM)
    vmem = pl.BlockSpec(memory_space=pltpu.VMEM)
    return pl.pallas_call(
        gather_kernel,
        out_shape=(
            pltpu.VMEM((512, HEAD_DIM), bf16),
            pltpu.VMEM((128, HEAD_DIM), bf16),
            pltpu.VMEM((128, HEAD_DIM), bf16),
            pltpu.VMEM((9, 2, 512, HEAD_DIM), bf16),
        ),
        in_specs=[anywhere] * 6,
        out_specs=(vmem,) * 4,
        scratch_shapes=[
            pltpu.VMEM((RING, 128, 512), bf16),
            pltpu.VMEM((RING, 128, 512), bf16),
            pltpu.VMEM((4096, 768), bf16),
            pltpu.VMEM((128, 768), f32),
            pltpu.VMEM((3, 2, 512, HEAD_DIM), bf16),
            dma((2,)), dma((2,)),
            dma((2,)), dma((2, 4 * PIECES)), dma, dma((7,)),
            dma, dma, dma, dma, dma, dma, dma, dma,
            dma((4, SPLIT)), dma((SPLIT,)), dma, pltpu.SemaphoreType.REGULAR,
        ],
        compiler_params=pltpu.CompilerParams(
            collective_id=0, has_side_effects=True, vmem_limit_bytes=58 * 1024 * 1024
        ),
        name="gather",
    )(slice_rows, w_query, w_key, w_value, prefix_keys, prefix_values)


def scores_of(keys, queries):
    return lax.dot_general(
        keys, queries, (((1,), (1,)), ((), ())), preferred_element_type=jnp.float32
    )


def weigh(values, weights):
    return lax.dot_general(
        values, weights, (((0,), (0,)), ((), ())), preferred_element_type=jnp.float32
    )


def attend_kernel(pb_ref, q_ref, k_ref, v_ref, kv_ref, out_ref, scores, m_ref, l_ref, o_ref):
    section = lax.axis_index("section")
    factor = math.log2(math.e) / math.sqrt(HEAD_DIM)
    never = 1e30
    queries = q_ref[...]

    def slot_of(offset):
        return 8 if offset == 0 else lax.rem(section - offset + 64, 8)

    key_row = lax.broadcasted_iota(jnp.int32, (128, 512), 0)
    query_row = lax.broadcasted_iota(jnp.int32, (128, 512), 1) % 128
    own = jnp.where(key_row <= query_row, scores_of(k_ref[...], queries), -never)
    top = jnp.max(own, axis=0, keepdims=True)
    for offset in range(REACH + 1):
        part = scores_of(kv_ref[slot_of(offset), 0, :BLOCK, :], queries)
        scores[offset] = part
        peak = jnp.max(part, axis=0, keepdims=True)
        top = jnp.maximum(top, jnp.where(section >= offset, peak, -never))
    weights = jnp.exp2((own - top) * factor)
    total = jnp.sum(weights, axis=0, keepdims=True)
    result = weigh(v_ref[...], weights.astype(jnp.bfloat16))
    for offset in range(REACH + 1):
        shift = jnp.where(section >= offset, top, never)
        weights = jnp.exp2((scores[offset] - shift) * factor)
        total += jnp.sum(weights, axis=0, keepdims=True)
        result += weigh(kv_ref[slot_of(offset), 1, :BLOCK, :], weights.astype(jnp.bfloat16))
    m_ref[...] = top
    l_ref[...] = total
    o_ref[...] = result

    for offset in range(REACH + 1):
        blocks = pb_ref[jnp.maximum(section - offset, 0)]

        @pl.when((section >= offset) & (blocks > 1))
        def _():
            part = scores_of(kv_ref[slot_of(offset), 0, BLOCK:, :], queries)
            before = m_ref[...]
            after = jnp.maximum(before, jnp.max(part, axis=0, keepdims=True))
            keep = jnp.exp2((before - after) * factor)
            weights = jnp.exp2((part - after) * factor)
            m_ref[...] = after
            l_ref[...] = l_ref[...] * keep + jnp.sum(weights, axis=0, keepdims=True)
            o_ref[...] = o_ref[...] * keep + weigh(
                kv_ref[slot_of(offset), 1, BLOCK:, :], weights.astype(jnp.bfloat16)
            )

    final = o_ref[...] / l_ref[...]
    for group in range(4):
        part = final[:, group * 128 : (group + 1) * 128]
        out_ref[:, group * 128 : (group + 1) * 128] = part.T.astype(jnp.bfloat16)


def attend(prefix_blocks, queries, own_keys, own_values, kv):
    vmem = pl.BlockSpec(memory_space=pltpu.VMEM)
    return pl.pallas_call(
        attend_kernel,
        out_shape=jax.ShapeDtypeStruct((128, 512), jnp.bfloat16),
        in_specs=[pl.BlockSpec(memory_space=pltpu.SMEM)] + [vmem] * 4,
        out_specs=vmem,
        scratch_shapes=[
            pltpu.VMEM((REACH + 1, BLOCK, 512), jnp.float32),
            pltpu.VMEM((1, 512), jnp.float32),
            pltpu.VMEM((1, 512), jnp.float32),
            pltpu.VMEM((HEAD_DIM, 512), jnp.float32),
        ],
        compiler_params=pltpu.CompilerParams(vmem_limit_bytes=24 * 1024 * 1024),
        name="attend",
    )(prefix_blocks, queries, own_keys, own_values, kv)


def on_device(slice_rows, w_query, w_key, w_value, prefix_keys, prefix_values, prefix_blocks):
    queries, own_keys, own_values, kv = gather(
        slice_rows, w_query, w_key, w_value, prefix_keys, prefix_values
    )
    return attend(prefix_blocks, queries, own_keys, own_values, kv)


def solution(mesh):
    in_specs = (
        P("section", "head"),
        P(None, "head"),
        P(None, "head"),
        P(None, "head"),
        P("section", "head"),
        P("section", "head"),
        P(),
    )
    out_specs = P("section", "head")
    return jax.shard_map(
        on_device, mesh=mesh, in_specs=in_specs, out_specs=out_specs, check_vma=False
    )
```

```python
import functools
import math

import jax
import jax.numpy as jnp
from jax import lax
from jax.experimental import pallas as pl
from jax.experimental.pallas import tpu as pltpu
from jax.sharding import PartitionSpec as P

HEAD_DIM = 128
BLOCK = 256
REACH = 7
COLUMNS = 4
LAYERS = 8
RING = 8
MESH = pl.DeviceIdType.MESH

SPLIT = 8
ROWS = 2 * 512 // SPLIT
LOW, HIGH = tuple(range(SPLIT // 2)), tuple(range(SPLIT // 2, SPLIT))
LOW_FIRST, HIGH_FIRST = LOW + HIGH, HIGH + LOW
RELAY = 4
PIECES = 8
PIECE = 128 // PIECES


def clock(hop, piece):
    return 3.5 + 2.75 * hop + 2.75 / PIECES * piece


DEFERRED = clock(0, PIECES - 1)


def rows_of(piece):
    return pl.ds((piece // 2) * ROWS, ROWS)


def steps(first, each=5.6 / SPLIT):
    return [first + each * index for index in range(SPLIT)]


def arrivals(column):
    events = []

    def add(times, slot, order=LOW_FIRST, kinds=(0, 1), right=(), left=(), up=(), pair=True, prev=None):
        for time, piece in zip(times, order):
            events.append(
                dict(
                    time=time, slot=slot, kinds=kinds, piece=piece,
                    right=piece in right, left=piece in left, up=piece in up, pair=pair,
                    prev=slot >= column if prev is None else prev,
                )
            )

    every = LOW + HIGH
    direct, relayed = steps(3.5), steps(6.5)
    if column < 3:
        add(steps(7.0, 2.8 / SPLIT), column, kinds=(1,))
        order = HIGH_FIRST if column == 2 else LOW_FIRST
        add(direct, RELAY, order, up=every, pair=False, prev=False)
    if column == 0:
        add(relayed, 1)
        add(steps(7.1), 3, right=LOW)
        add(steps(8.3), 2)
    elif column == 1:
        add(direct, 0, right=LOW)
        add(relayed, 2, left=every)
        add(steps(9.5), 3, LOW)
        add(steps(8.3), 3, HIGH)
    elif column == 2:
        add(direct, 1, right=every)
        add(relayed, 3, HIGH_FIRST, left=HIGH)
        add(steps(8.0), 0, LOW)
        add(steps(8.0), 0, HIGH)
    else:
        add(steps(4.2), 3, right=every)
        add(direct, 2)
        add(direct, 0, HIGH_FIRST, left=HIGH)
        add(steps(8.0), 1)
    return sorted(events, key=lambda event: event["time"])


def gather_kernel(
    x_ref, wq_ref, wk_ref, wv_ref, pk_ref, pv_ref,
    q_ref, k_ref, v_ref, kv_ref,
    xbuf, xother, weights, acc, relay,
    w_sem, local_sem, x_send, x_recv, x_pair_send, x_pair_recv,
    right_send, left_send, up_send, own_send, relay_send, right_fwd, left_fwd, pair_send,
    slot_recv, relay_recv, pair_recv, ready,
):
    section = lax.axis_index("section")
    y = lax.axis_index("head")
    core = lax.rem(section, 2)
    x = lax.rem(lax.div(section, 2), COLUMNS)
    z = lax.div(section, 2 * COLUMNS)

    def at(layer, column, kind, ring=None):
        return ((layer * COLUMNS + column) * 2 + kind, y if ring is None else ring)

    x_right, x_left = lax.rem(x + 1, COLUMNS), lax.rem(x + COLUMNS - 1, COLUMNS)
    z_above, z_below = lax.rem(z + 1, LAYERS), lax.rem(z + LAYERS - 1, LAYERS)
    y_up, y_down = lax.rem(y + 1, RING), lax.rem(y + RING - 1, RING)
    right, left = at(z, x_right, 1), at(z, x_left, 1)
    above = at(z_above, x, 1)
    ways = (at(z, x, 1, y_up), at(z, x, 1, y_down))
    pair = at(z, x, 1 - core)

    def block_at(hop):
        return lax.rem(y + hop + RING, RING)

    visits = [0, -1, 1, -2, 2, -3, 3, 4]

    def start_weights(hop):
        start = pl.multiple_of(block_at(hop) * 512, 512)
        rows = pl.ds(start, 512)
        for source, first, size in ((wq_ref, 0, 512), (wk_ref, 512, 128), (wv_ref, 640, 128)):
            pltpu.make_async_copy(
                source.at[rows], weights.at[rows, first : first + size], w_sem.at[min(abs(hop), 1)]
            ).start()

    def wait_weights(index, blocks):
        rows = weights.at[: blocks * 512]
        pltpu.make_async_copy(rows, rows, w_sem.at[index]).wait()

    def project(hop):
        start = pl.multiple_of(block_at(hop) * 512, 512)
        part = jnp.dot(
            xbuf[block_at(hop)], weights[pl.ds(start, 512), :], preferred_element_type=jnp.float32
        )
        if hop == 0:
            acc[...] = part
        else:
            acc[...] += part

    def remote(source, target, send, recv, device):
        return pltpu.make_async_remote_copy(
            src_ref=source, dst_ref=target, send_sem=send, recv_sem=recv,
            device_id=device, device_id_type=MESH,
        )

    own_x = pltpu.make_async_copy(x_ref, xbuf.at[y], local_sem.at[0])
    own_x.start()
    start_weights(0)

    def tell(semaphore, device):
        pl.semaphore_signal(semaphore, inc=1, device_id=device, device_id_type=MESH)

    barrier = pltpu.get_barrier_semaphore()

    @pl.when(core == 1)
    def _():
        for kind in range(2):
            for device in (
                at(z, x, kind, y_up), at(z, x, kind, y_down),
                at(z, x_right, kind), at(z, x_left, kind),
            ):
                tell(barrier, device)

    tell(barrier, pair)

    @pl.when((z < LAYERS - 1) & ((core == 1) | (x == 3)))
    def _():
        tell(barrier, above)

    for hop in visits[1:]:
        start_weights(hop)
    pltpu.make_async_copy(pk_ref, kv_ref.at[8, 0], local_sem.at[1]).start()
    pltpu.make_async_copy(pv_ref, kv_ref.at[8, 1], local_sem.at[1]).start()
    below_count = jnp.where((core == 1) & (z > 0), jnp.where(x == 3, 2, 1), 0)
    pl.semaphore_wait(barrier, 5 + below_count)

    @pl.when((core == 1) & (z > 0))
    def _():
        tell(ready, at(z_below, x, 1))

        @pl.when(x == 3)
        def _():
            tell(ready, at(z_below, x, 0))

    def received(here, semaphore):
        remote(here, here, own_send, semaphore, pair).wait_recv()

    def sent(here, semaphore):
        remote(here, here, semaphore, pair_recv, pair).wait_send()

    def pieces_of(count):
        return kv_ref.at[0, 0, : ROWS * count] if count < 3 else kv_ref.at[: count // SPLIT]

    def rows_at(piece):
        return pl.ds(piece * PIECE, PIECE)

    def x_own(way, piece, kind):
        target = xother if kind == 0 else xbuf
        return remote(
            x_ref.at[rows_at(piece)], target.at[y, rows_at(piece)],
            x_send.at[way], x_recv.at[way, piece], ways[way],
        )

    def x_origin(way, hop):
        return block_at(-hop - 1 if way == 0 else hop + 1)

    def x_piece(way, hop, piece, kind):
        return (xother if kind == 0 else xbuf).at[x_origin(way, hop), rows_at(piece)]

    def x_forward(way, hop, piece, kind):
        here = x_piece(way, hop, piece, kind)
        index = (hop + 1) * PIECES + piece
        return remote(here, here, x_send.at[way], x_recv.at[way, index], ways[way])

    def x_hand(way, hop, piece):
        rows = rows_at(piece)
        return remote(
            xother.at[x_origin(way, hop), rows], xbuf.at[x_origin(way, hop), rows],
            x_pair_send, x_pair_recv.at[min(hop * 2 + way, 6)], pair,
        )

    def travels(way, hop, piece):
        return hop < 3 or (hop == 3 and piece // (PIECES // 2) == way)

    def own_piece(piece):
        return (pk_ref if piece % 2 == 0 else pv_ref).at[rows_of(piece)]

    def slot_piece(column, kind, piece):
        return kv_ref.at[column * 2 + kind, piece % 2, rows_of(piece)]

    def relay_piece(kind, piece):
        return relay.at[kind, piece % 2, rows_of(piece)]

    def send_right(kind, piece, column):
        return remote(
            own_piece(piece), slot_piece(column, kind, piece),
            right_send, slot_recv.at[column, piece], right,
        )

    def send_left(kind, piece, column):
        if column == 0:
            target, arrived = slot_piece(0, kind, piece), slot_recv.at[0, piece]
        else:
            target, arrived = relay_piece(kind, piece), relay_recv.at[piece]
        return remote(own_piece(piece), target, left_send, arrived, left)

    def send_up(kind, piece):
        if kind == 0:
            target, arrived = relay_piece(2, piece), slot_recv.at[x, piece]
        else:
            target, arrived = slot_piece(x, 1, piece), slot_recv.at[x, piece]
        return remote(own_piece(piece), target, up_send, arrived, above)

    def send_pair(piece):
        return remote(
            own_piece(piece), slot_piece(x, 0, piece),
            own_send, pair_recv, pair,
        )

    def first_sends(kind, column):
        leftward = HIGH_FIRST if column in (0, 3) else LOW_FIRST
        for index in range(SPLIT):
            yield column > 0, functools.partial(send_left, kind, leftward[index], column)
            if column < 3:
                yield False, functools.partial(send_right, kind, index, column)

    def source_of(event, column, kind):
        if event["slot"] == RELAY:
            return relay_piece(kind, event["piece"])
        if column == 3 and event["slot"] == 3 and kind == 0:
            return relay_piece(2, event["piece"])
        return slot_piece(event["slot"], kind, event["piece"])

    def sends_of(event, column, upward):
        for kind in event["kinds"]:
            piece, slot = event["piece"], event["slot"]
            source = source_of(event, column, kind)
            if upward:
                if event["up"]:
                    yield remote(
                        source, slot_piece(column + 1, kind, piece), relay_send,
                        slot_recv.at[column + 1, piece], above,
                    )
                continue
            if slot == RELAY:
                continue
            target, arrived = slot_piece(slot, kind, piece), slot_recv.at[slot, piece]
            if event["right"]:
                yield remote(source, target, right_fwd, arrived, right)
            if event["left"]:
                yield remote(source, target, left_fwd, arrived, left)
            if event["pair"] and (slot != column or kind == 1):
                yield remote(source, target, pair_send, pair_recv, pair)

    def count(column, what, prevs):
        total = 0
        for event in arrivals(column):
            if event[what] and (prevs or not event["prev"]):
                kinds = (1,) if what == "pair" and event["slot"] == column else event["kinds"]
                total += len(kinds)
        return total

    def guarded(condition, run):
        if condition is None:
            run()
        else:
            pl.when(condition)(run)

    def start_first(kind):
        for piece in range(PIECES):
            for way in range(2):
                x_own(way, piece, kind).start()
        for column in range(COLUMNS):

            @pl.when(x == column)
            def _():
                plain = [make for needs, make in first_sends(kind, column) if not needs]
                needing = [make for needs, make in first_sends(kind, column) if needs]
                if needing:

                    @pl.when(z < LAYERS - 1)
                    def _():
                        for make in needing:
                            make().start()

                for make in plain:
                    make().start()

    def finish_first(kind):
        @pl.when((x == 0) | (z < LAYERS - 1))
        def _():
            sent(pieces_of(SPLIT), left_send)

        @pl.when(x < 3)
        def _():
            sent(pieces_of(SPLIT), right_send)

        @pl.when((z < LAYERS - 1) & (x == 3) if kind == 0 else z < LAYERS - 1)
        def _():
            sent(pieces_of(SPLIT), up_send)

    @pl.when(z == 0)
    def _():
        for column in range(COLUMNS):

            @pl.when(x == column)
            def _():
                for slot in range(column * 2 + 2, COLUMNS * 2):
                    kv_ref[slot] = jnp.zeros((2, 512, HEAD_DIM), jnp.bfloat16)

                @pl.when(core == 0)
                def _():
                    kv_ref[column * 2 + 1] = jnp.zeros((2, 512, HEAD_DIM), jnp.bfloat16)

    @pl.when(core == 0)
    def _():
        start_first(0)
        for piece in range(SPLIT):
            send_pair(piece).start()
        own_x.wait()
        wait_weights(0, 1)
        project(0)

        @pl.when((x == 3) & (z < LAYERS - 1))
        def _():
            pl.semaphore_wait(ready, 1)
            for piece in range(SPLIT):
                send_up(0, piece).start()

        wait_weights(1, 7)
        for index, hop in enumerate(visits[1:]):
            received(xbuf.at[0], x_pair_recv.at[index])
            project(hop)

        @pl.when(z > 0)
        def _():
            received(pieces_of(7 * SPLIT), pair_recv)

        for column in range(1, COLUMNS):

            @pl.when((z == 0) & (x == column))
            def _():
                received(pieces_of(2 * SPLIT * column), pair_recv)

        finish_first(0)
        sent(pieces_of(SPLIT), own_send)
        for way in range(2):
            sent(xbuf.at[0], x_send.at[way])

    schedules = [arrivals(column) for column in range(COLUMNS)]

    def handle(event, column):
        def run():
            semaphore = (relay_recv if event["slot"] == RELAY else slot_recv.at[event["slot"]]).at[event["piece"]]
            received(pieces_of(len(event["kinds"])), semaphore)
            if event["up"]:
                held = event["time"] <= DEFERRED

                @pl.when((z > 0) & (z < LAYERS - 1) if held else z < LAYERS - 1)
                def _():
                    for copy in sends_of(event, column, True):
                        copy.start()

            for copy in sends_of(event, column, False):
                copy.start()

        whole = event["slot"] == RELAY and event["up"]
        guarded(z < LAYERS - 1 if whole else z > 0 if event["prev"] else None, run)

    def prefixes(until):
        for column in range(COLUMNS):
            due = [event for event in schedules[column] if event["time"] <= until]
            if not due:
                continue
            schedules[column] = schedules[column][len(due) :]

            @pl.when(x == column)
            def _():
                for event in due:
                    handle(event, column)

    def lowest_goes_up():
        @pl.when(z == 0)
        def _():
            pl.semaphore_wait(ready, 1)
            for piece in range(SPLIT):
                send_up(1, piece).start()

    def lowest_relays():
        for column in range(0, COLUMNS - 1):

            @pl.when((z == 0) & (x == column))
            def _():
                for event in arrivals(column):
                    if event["up"] and event["time"] <= DEFERRED:
                        for copy in sends_of(event, column, True):
                            copy.start()

    @pl.when(core == 1)
    def _():
        start_first(1)

        @pl.when((z > 0) & (z < LAYERS - 1))
        def _():
            pl.semaphore_wait(ready, 1)
            for piece in range(SPLIT):
                send_up(1, piece).start()

        own_x.wait()
        wait_weights(0, 1)
        project(0)
        lowest_goes_up()
        for hop in range(4):
            for piece in range(PIECES):
                if hop == 3 and piece >= PIECES // 2:
                    continue
                for way in range(2):
                    this = piece if hop < 3 or way == 0 else piece + PIECES // 2
                    received(xbuf.at[0, : 2 * PIECE], x_recv.at[way, hop * PIECES + this])
                    for kind in range(2):
                        if travels(way, hop + 1, this):
                            x_forward(way, hop, this, kind).start()
                    x_hand(way, hop, this).start()
                prefixes(clock(hop, piece))
                if hop == 0 and piece == PIECES - 1:
                    lowest_relays()
                    wait_weights(1, 7)
                if hop > 0 and piece == 0:
                    project(-hop)
                if hop > 0 and piece == 1:
                    project(hop)
        project(4)
        prefixes(99.0)
        received(pieces_of(SPLIT), pair_recv)

        finish_first(1)
        for way in range(2):
            sent(xbuf.at[:6], x_send.at[way])
        sent(xbuf.at[:7], x_pair_send)
        for column in range(COLUMNS):

            @pl.when(x == column)
            def _():
                for condition, prevs in ((z > 0, True), (z == 0, False)):

                    @pl.when(condition)
                    def _():
                        for what, semaphore in (("pair", pair_send), ("right", right_fwd), ("left", left_fwd)):
                            total = count(column, what, prevs)
                            if total:
                                sent(pieces_of(total), semaphore)

                if column < 3:

                    @pl.when(z < LAYERS - 1)
                    def _():
                        sent(pieces_of(2 * SPLIT), relay_send)

    for group in range(4):
        q_ref[group * 128 : (group + 1) * 128, :] = acc[:, group * 128 : (group + 1) * 128].astype(jnp.bfloat16)
    k_ref[...] = acc[:, 512:640].astype(jnp.bfloat16)
    v_ref[...] = acc[:, 640:768].astype(jnp.bfloat16)
    pltpu.make_async_copy(kv_ref.at[8], kv_ref.at[8], local_sem.at[1]).wait()


def gather(slice_rows, w_query, w_key, w_value, prefix_keys, prefix_values):
    bf16, f32 = jnp.bfloat16, jnp.float32
    dma = pltpu.SemaphoreType.DMA
    anywhere = pl.BlockSpec(memory_space=pltpu.HBM)
    vmem = pl.BlockSpec(memory_space=pltpu.VMEM)
    return pl.pallas_call(
        gather_kernel,
        out_shape=(
            pltpu.VMEM((512, HEAD_DIM), bf16),
            pltpu.VMEM((128, HEAD_DIM), bf16),
            pltpu.VMEM((128, HEAD_DIM), bf16),
            pltpu.VMEM((9, 2, 512, HEAD_DIM), bf16),
        ),
        in_specs=[anywhere] * 6,
        out_specs=(vmem,) * 4,
        scratch_shapes=[
            pltpu.VMEM((RING, 128, 512), bf16),
            pltpu.VMEM((RING, 128, 512), bf16),
            pltpu.VMEM((4096, 768), bf16),
            pltpu.VMEM((128, 768), f32),
            pltpu.VMEM((3, 2, 512, HEAD_DIM), bf16),
            dma((2,)), dma((2,)),
            dma((2,)), dma((2, 4 * PIECES)), dma, dma((7,)),
            dma, dma, dma, dma, dma, dma, dma, dma,
            dma((4, SPLIT)), dma((SPLIT,)), dma, pltpu.SemaphoreType.REGULAR,
        ],
        compiler_params=pltpu.CompilerParams(
            collective_id=0, has_side_effects=True, vmem_limit_bytes=58 * 1024 * 1024
        ),
        name="gather",
    )(slice_rows, w_query, w_key, w_value, prefix_keys, prefix_values)


def scores_of(keys, queries):
    return lax.dot_general(
        keys, queries, (((1,), (1,)), ((), ())), preferred_element_type=jnp.float32
    )


def weigh(values, weights):
    return lax.dot_general(
        values, weights, (((0,), (0,)), ((), ())), preferred_element_type=jnp.float32
    )


def attend_kernel(
    blocks_ref, q_ref, k_ref, v_ref, kv_ref, out_ref, scores, m_ref, l_ref, o_ref, pb_ref, out, pb_sem, out_sem
):
    section = lax.axis_index("section")
    factor = math.log2(math.e) / math.sqrt(HEAD_DIM)
    never = 1e30
    live = pltpu.make_async_copy(blocks_ref, pb_ref, pb_sem)
    live.start()
    queries = q_ref[...]

    def slot_of(offset):
        return 8 if offset == 0 else lax.rem(section - offset + 64, 8)

    key_row = lax.broadcasted_iota(jnp.int32, (128, 512), 0)
    query_row = lax.broadcasted_iota(jnp.int32, (128, 512), 1) % 128
    own = jnp.where(key_row <= query_row, scores_of(k_ref[...], queries), -never)
    top = jnp.max(own, axis=0, keepdims=True)
    for offset in range(REACH + 1):
        part = scores_of(kv_ref[slot_of(offset), 0, :BLOCK, :], queries)
        scores[offset] = part
        peak = jnp.max(part, axis=0, keepdims=True)
        top = jnp.maximum(top, jnp.where(section >= offset, peak, -never))
    weights = jnp.exp2((own - top) * factor)
    total = jnp.sum(weights, axis=0, keepdims=True)
    result = weigh(v_ref[...], weights.astype(jnp.bfloat16))
    for offset in range(REACH + 1):
        shift = jnp.where(section >= offset, top, never)
        weights = jnp.exp2((scores[offset] - shift) * factor)
        total += jnp.sum(weights, axis=0, keepdims=True)
        result += weigh(kv_ref[slot_of(offset), 1, :BLOCK, :], weights.astype(jnp.bfloat16))
    m_ref[...] = top
    l_ref[...] = total
    o_ref[...] = result
    live.wait()

    for offset in range(REACH + 1):
        blocks = pb_ref[jnp.maximum(section - offset, 0)]

        @pl.when((section >= offset) & (blocks > 1))
        def _():
            part = scores_of(kv_ref[slot_of(offset), 0, BLOCK:, :], queries)
            before = m_ref[...]
            after = jnp.maximum(before, jnp.max(part, axis=0, keepdims=True))
            keep = jnp.exp2((before - after) * factor)
            weights = jnp.exp2((part - after) * factor)
            m_ref[...] = after
            l_ref[...] = l_ref[...] * keep + jnp.sum(weights, axis=0, keepdims=True)
            o_ref[...] = o_ref[...] * keep + weigh(
                kv_ref[slot_of(offset), 1, BLOCK:, :], weights.astype(jnp.bfloat16)
            )

    final = o_ref[...] / l_ref[...]
    for group in range(4):
        columns = slice(group * 128, (group + 1) * 128)
        out[:, columns] = final[:, columns].T.astype(jnp.bfloat16)
    copy = pltpu.make_async_copy(out, out_ref, out_sem)
    copy.start()
    copy.wait()


def attend(prefix_blocks, queries, own_keys, own_values, kv):
    vmem = pl.BlockSpec(memory_space=pltpu.VMEM)
    return pl.pallas_call(
        attend_kernel,
        out_shape=jax.ShapeDtypeStruct((128, 512), jnp.bfloat16),
        in_specs=[pl.BlockSpec(memory_space=pltpu.HBM)] + [vmem] * 4,
        out_specs=pl.BlockSpec(memory_space=pltpu.HBM),
        scratch_shapes=[
            pltpu.VMEM((REACH + 1, BLOCK, 512), jnp.float32),
            pltpu.VMEM((1, 512), jnp.float32),
            pltpu.VMEM((1, 512), jnp.float32),
            pltpu.VMEM((HEAD_DIM, 512), jnp.float32),
            pltpu.SMEM((64,), jnp.int32),
            pltpu.VMEM((128, 512), jnp.bfloat16),
            pltpu.SemaphoreType.DMA,
            pltpu.SemaphoreType.DMA,
        ],
        compiler_params=pltpu.CompilerParams(vmem_limit_bytes=24 * 1024 * 1024),
        name="attend",
    )(prefix_blocks, queries, own_keys, own_values, kv)


def on_device(slice_rows, w_query, w_key, w_value, prefix_keys, prefix_values, prefix_blocks):
    queries, own_keys, own_values, kv = gather(
        slice_rows, w_query, w_key, w_value, prefix_keys, prefix_values
    )
    return attend(prefix_blocks, queries, own_keys, own_values, kv)


def solution(mesh):
    in_specs = (
        P("section", "head"),
        P(None, "head"),
        P(None, "head"),
        P(None, "head"),
        P("section", "head"),
        P("section", "head"),
        P(),
    )
    out_specs = P("section", "head")
    return jax.shard_map(
        on_device, mesh=mesh, in_specs=in_specs, out_specs=out_specs, check_vma=False
    )
```

```python
import functools
import math

import jax
import jax.numpy as jnp
from jax import lax
from jax.experimental import pallas as pl
from jax.experimental.pallas import tpu as pltpu
from jax.sharding import PartitionSpec as P

HEAD_DIM = 128
BLOCK = 256
REACH = 7
COLUMNS = 4
LAYERS = 8
RING = 8
MESH = pl.DeviceIdType.MESH

SPLIT = 8
ROWS = 2 * 512 // SPLIT
LOW, HIGH = tuple(range(SPLIT // 2)), tuple(range(SPLIT // 2, SPLIT))
LOW_FIRST, HIGH_FIRST = LOW + HIGH, HIGH + LOW
RELAY = 4
PIECES = 8
PIECE = 128 // PIECES


def clock(hop, piece):
    return 3.5 + 2.75 * hop + 2.75 / PIECES * piece


DEFERRED = clock(0, PIECES - 1)


def rows_of(piece):
    return pl.ds((piece // 2) * ROWS, ROWS)


def steps(first, each=5.6 / SPLIT):
    return [first + each * index for index in range(SPLIT)]


def arrivals(column):
    events = []

    def add(times, slot, order=LOW_FIRST, kinds=(0, 1), right=(), left=(), up=(), pair=True, prev=None):
        for time, piece in zip(times, order):
            events.append(
                dict(
                    time=time, slot=slot, kinds=kinds, piece=piece,
                    right=piece in right, left=piece in left, up=piece in up, pair=pair,
                    prev=slot >= column if prev is None else prev,
                )
            )

    every = LOW + HIGH
    direct, relayed = steps(3.5), steps(6.5)
    if column < 3:
        add(steps(7.0, 2.8 / SPLIT), column, kinds=(1,))
        order = HIGH_FIRST if column == 2 else LOW_FIRST
        add(direct, RELAY, order, up=every, pair=False, prev=False)
    if column == 0:
        add(relayed, 1)
        add(steps(7.1), 3, right=LOW)
        add(steps(8.3), 2)
    elif column == 1:
        add(direct, 0, right=LOW)
        add(relayed, 2, left=every)
        add(steps(9.5), 3, LOW)
        add(steps(8.3), 3, HIGH)
    elif column == 2:
        add(direct, 1, right=every)
        add(relayed, 3, HIGH_FIRST, left=HIGH)
        add(steps(8.0), 0, LOW)
        add(steps(8.0), 0, HIGH)
    else:
        add(steps(4.2), 3, right=every)
        add(direct, 2)
        add(direct, 0, HIGH_FIRST, left=HIGH)
        add(steps(8.0), 1)
    return sorted(events, key=lambda event: event["time"])


def gather_kernel(
    x_ref, wq_ref, wk_ref, wv_ref, pk_ref, pv_ref,
    q_ref, k_ref, v_ref, kv_ref,
    xbuf, xother, weights, acc, relay,
    w_sem, local_sem, x_send, x_recv, x_pair_send, x_pair_recv,
    right_send, left_send, up_send, own_send, relay_send, right_fwd, left_fwd, pair_send,
    slot_recv, relay_recv, pair_recv, ready,
):
    section = lax.axis_index("section")
    y = lax.axis_index("head")
    core = lax.rem(section, 2)
    x = lax.rem(lax.div(section, 2), COLUMNS)
    z = lax.div(section, 2 * COLUMNS)

    def at(layer, column, kind, ring=None):
        return ((layer * COLUMNS + column) * 2 + kind, y if ring is None else ring)

    x_right, x_left = lax.rem(x + 1, COLUMNS), lax.rem(x + COLUMNS - 1, COLUMNS)
    z_above, z_below = lax.rem(z + 1, LAYERS), lax.rem(z + LAYERS - 1, LAYERS)
    y_up, y_down = lax.rem(y + 1, RING), lax.rem(y + RING - 1, RING)
    right, left = at(z, x_right, 1), at(z, x_left, 1)
    above = at(z_above, x, 1)
    ways = (at(z, x, 1, y_up), at(z, x, 1, y_down))
    pair = at(z, x, 1 - core)

    def block_at(hop):
        return lax.rem(y + hop + RING, RING)

    visits = [0, -1, 1, -2, 2, -3, 3, 4]

    def start_weights(hop):
        start = pl.multiple_of(block_at(hop) * 512, 512)
        rows = pl.ds(start, 512)
        for source, first, size in ((wq_ref, 0, 512), (wk_ref, 512, 128), (wv_ref, 640, 128)):
            pltpu.make_async_copy(
                source.at[rows], weights.at[rows, first : first + size], w_sem.at[min(abs(hop), 1)]
            ).start()

    def wait_weights(index, blocks):
        rows = weights.at[: blocks * 512]
        pltpu.make_async_copy(rows, rows, w_sem.at[index]).wait()

    def project(hop):
        start = pl.multiple_of(block_at(hop) * 512, 512)
        part = jnp.dot(
            xbuf[block_at(hop)], weights[pl.ds(start, 512), :], preferred_element_type=jnp.float32
        )
        if hop == 0:
            acc[...] = part
        else:
            acc[...] += part

    def write_projected():
        for group in range(4):
            q_ref[group * 128 : (group + 1) * 128, :] = acc[:, group * 128 : (group + 1) * 128].astype(jnp.bfloat16)
        k_ref[...] = acc[:, 512:640].astype(jnp.bfloat16)
        v_ref[...] = acc[:, 640:768].astype(jnp.bfloat16)

    def remote(source, target, send, recv, device):
        return pltpu.make_async_remote_copy(
            src_ref=source, dst_ref=target, send_sem=send, recv_sem=recv,
            device_id=device, device_id_type=MESH,
        )

    own_x = pltpu.make_async_copy(x_ref, xbuf.at[y], local_sem.at[0])
    own_x.start()
    start_weights(0)

    def tell(semaphore, device):
        pl.semaphore_signal(semaphore, inc=1, device_id=device, device_id_type=MESH)

    barrier = pltpu.get_barrier_semaphore()

    @pl.when(core == 1)
    def _():
        for kind in range(2):
            for device in (
                at(z, x, kind, y_up), at(z, x, kind, y_down),
                at(z, x_right, kind), at(z, x_left, kind),
            ):
                tell(barrier, device)

    tell(barrier, pair)

    @pl.when((z < LAYERS - 1) & ((core == 1) | (x == 3)))
    def _():
        tell(barrier, above)

    for hop in visits[1:]:
        start_weights(hop)
    pltpu.make_async_copy(pk_ref, kv_ref.at[8, 0], local_sem.at[1]).start()
    pltpu.make_async_copy(pv_ref, kv_ref.at[8, 1], local_sem.at[1]).start()
    below_count = jnp.where((core == 1) & (z > 0), jnp.where(x == 3, 2, 1), 0)
    pl.semaphore_wait(barrier, 5 + below_count)

    @pl.when((core == 1) & (z > 0))
    def _():
        tell(ready, at(z_below, x, 1))

        @pl.when(x == 3)
        def _():
            tell(ready, at(z_below, x, 0))

    def received(here, semaphore):
        remote(here, here, own_send, semaphore, pair).wait_recv()

    def sent(here, semaphore):
        remote(here, here, semaphore, pair_recv, pair).wait_send()

    def pieces_of(count):
        return kv_ref.at[0, 0, : ROWS * count] if count < 3 else kv_ref.at[: count // SPLIT]

    def rows_at(piece):
        return pl.ds(piece * PIECE, PIECE)

    def x_own(way, piece, kind):
        target = xother if kind == 0 else xbuf
        return remote(
            x_ref.at[rows_at(piece)], target.at[y, rows_at(piece)],
            x_send.at[way], x_recv.at[way, piece], ways[way],
        )

    def x_origin(way, hop):
        return block_at(-hop - 1 if way == 0 else hop + 1)

    def x_piece(way, hop, piece, kind):
        return (xother if kind == 0 else xbuf).at[x_origin(way, hop), rows_at(piece)]

    def x_forward(way, hop, piece, kind):
        here = x_piece(way, hop, piece, kind)
        index = (hop + 1) * PIECES + piece
        return remote(here, here, x_send.at[way], x_recv.at[way, index], ways[way])

    def x_hand(way, hop, piece):
        rows = rows_at(piece)
        return remote(
            xother.at[x_origin(way, hop), rows], xbuf.at[x_origin(way, hop), rows],
            x_pair_send, x_pair_recv.at[min(hop * 2 + way, 6)], pair,
        )

    def travels(way, hop, piece):
        return hop < 3 or (hop == 3 and piece // (PIECES // 2) == way)

    def own_piece(piece):
        return (pk_ref if piece % 2 == 0 else pv_ref).at[rows_of(piece)]

    def slot_piece(column, kind, piece):
        return kv_ref.at[column * 2 + kind, piece % 2, rows_of(piece)]

    def relay_piece(kind, piece):
        return relay.at[kind, piece % 2, rows_of(piece)]

    def send_right(kind, piece, column):
        return remote(
            own_piece(piece), slot_piece(column, kind, piece),
            right_send, slot_recv.at[column, piece], right,
        )

    def send_left(kind, piece, column):
        if column == 0:
            target, arrived = slot_piece(0, kind, piece), slot_recv.at[0, piece]
        else:
            target, arrived = relay_piece(kind, piece), relay_recv.at[piece]
        return remote(own_piece(piece), target, left_send, arrived, left)

    def send_up(kind, piece):
        if kind == 0:
            target, arrived = relay_piece(2, piece), slot_recv.at[x, piece]
        else:
            target, arrived = slot_piece(x, 1, piece), slot_recv.at[x, piece]
        return remote(own_piece(piece), target, up_send, arrived, above)

    def send_pair(piece):
        return remote(
            own_piece(piece), slot_piece(x, 0, piece),
            own_send, pair_recv, pair,
        )

    def first_sends(kind, column):
        leftward = HIGH_FIRST if column in (0, 3) else LOW_FIRST
        for index in range(SPLIT):
            yield column > 0, functools.partial(send_left, kind, leftward[index], column)
            if column < 3:
                yield False, functools.partial(send_right, kind, index, column)

    def source_of(event, column, kind):
        if event["slot"] == RELAY:
            return relay_piece(kind, event["piece"])
        if column == 3 and event["slot"] == 3 and kind == 0:
            return relay_piece(2, event["piece"])
        return slot_piece(event["slot"], kind, event["piece"])

    def sends_of(event, column, upward):
        for kind in event["kinds"]:
            piece, slot = event["piece"], event["slot"]
            source = source_of(event, column, kind)
            if upward:
                if event["up"]:
                    yield remote(
                        source, slot_piece(column + 1, kind, piece), relay_send,
                        slot_recv.at[column + 1, piece], above,
                    )
                continue
            if slot == RELAY:
                continue
            target, arrived = slot_piece(slot, kind, piece), slot_recv.at[slot, piece]
            if event["right"]:
                yield remote(source, target, right_fwd, arrived, right)
            if event["left"]:
                yield remote(source, target, left_fwd, arrived, left)
            if event["pair"] and (slot != column or kind == 1):
                yield remote(source, target, pair_send, pair_recv, pair)

    def count(column, what, prevs):
        total = 0
        for event in arrivals(column):
            if event[what] and (prevs or not event["prev"]):
                kinds = (1,) if what == "pair" and event["slot"] == column else event["kinds"]
                total += len(kinds)
        return total

    def guarded(condition, run):
        if condition is None:
            run()
        else:
            pl.when(condition)(run)

    def start_first(kind):
        for piece in range(PIECES):
            for way in range(2):
                x_own(way, piece, kind).start()
        for column in range(COLUMNS):

            @pl.when(x == column)
            def _():
                plain = [make for needs, make in first_sends(kind, column) if not needs]
                needing = [make for needs, make in first_sends(kind, column) if needs]
                if needing:

                    @pl.when(z < LAYERS - 1)
                    def _():
                        for make in needing:
                            make().start()

                for make in plain:
                    make().start()

    def finish_first(kind):
        @pl.when((x == 0) | (z < LAYERS - 1))
        def _():
            sent(pieces_of(SPLIT), left_send)

        @pl.when(x < 3)
        def _():
            sent(pieces_of(SPLIT), right_send)

        @pl.when((z < LAYERS - 1) & (x == 3) if kind == 0 else z < LAYERS - 1)
        def _():
            sent(pieces_of(SPLIT), up_send)

    @pl.when(z == 0)
    def _():
        for column in range(COLUMNS):

            @pl.when(x == column)
            def _():
                for slot in range(column * 2 + 2, COLUMNS * 2):
                    kv_ref[slot] = jnp.zeros((2, 512, HEAD_DIM), jnp.bfloat16)

                @pl.when(core == 0)
                def _():
                    kv_ref[column * 2 + 1] = jnp.zeros((2, 512, HEAD_DIM), jnp.bfloat16)

    @pl.when(core == 0)
    def _():
        start_first(0)
        for piece in range(SPLIT):
            send_pair(piece).start()
        own_x.wait()
        wait_weights(0, 1)
        project(0)

        @pl.when((x == 3) & (z < LAYERS - 1))
        def _():
            pl.semaphore_wait(ready, 1)
            for piece in range(SPLIT):
                send_up(0, piece).start()

        wait_weights(1, 7)
        for index, hop in enumerate(visits[1:]):
            received(xbuf.at[0], x_pair_recv.at[index])
            project(hop)
        write_projected()

        @pl.when(z > 0)
        def _():
            received(pieces_of(7 * SPLIT), pair_recv)

        for column in range(1, COLUMNS):

            @pl.when((z == 0) & (x == column))
            def _():
                received(pieces_of(2 * SPLIT * column), pair_recv)

        finish_first(0)
        sent(pieces_of(SPLIT), own_send)
        for way in range(2):
            sent(xbuf.at[0], x_send.at[way])

    schedules = [arrivals(column) for column in range(COLUMNS)]

    def handle(event, column):
        def run():
            semaphore = (relay_recv if event["slot"] == RELAY else slot_recv.at[event["slot"]]).at[event["piece"]]
            received(pieces_of(len(event["kinds"])), semaphore)
            if event["up"]:
                held = event["time"] <= DEFERRED

                @pl.when((z > 0) & (z < LAYERS - 1) if held else z < LAYERS - 1)
                def _():
                    for copy in sends_of(event, column, True):
                        copy.start()

            for copy in sends_of(event, column, False):
                copy.start()

        whole = event["slot"] == RELAY and event["up"]
        guarded(z < LAYERS - 1 if whole else z > 0 if event["prev"] else None, run)

    def prefixes(until):
        for column in range(COLUMNS):
            due = [event for event in schedules[column] if event["time"] <= until]
            if not due:
                continue
            schedules[column] = schedules[column][len(due) :]

            @pl.when(x == column)
            def _():
                for event in due:
                    handle(event, column)

    def lowest_goes_up():
        @pl.when(z == 0)
        def _():
            pl.semaphore_wait(ready, 1)
            for piece in range(SPLIT):
                send_up(1, piece).start()

    def lowest_relays():
        for column in range(0, COLUMNS - 1):

            @pl.when((z == 0) & (x == column))
            def _():
                for event in arrivals(column):
                    if event["up"] and event["time"] <= DEFERRED:
                        for copy in sends_of(event, column, True):
                            copy.start()

    @pl.when(core == 1)
    def _():
        start_first(1)

        @pl.when((z > 0) & (z < LAYERS - 1))
        def _():
            pl.semaphore_wait(ready, 1)
            for piece in range(SPLIT):
                send_up(1, piece).start()

        own_x.wait()
        wait_weights(0, 1)
        project(0)
        lowest_goes_up()
        for hop in range(4):
            for piece in range(PIECES):
                if hop == 3 and piece >= PIECES // 2:
                    continue
                for way in range(2):
                    this = piece if hop < 3 or way == 0 else piece + PIECES // 2
                    received(xbuf.at[0, : 2 * PIECE], x_recv.at[way, hop * PIECES + this])
                    for kind in range(2):
                        if travels(way, hop + 1, this):
                            x_forward(way, hop, this, kind).start()
                    x_hand(way, hop, this).start()
                prefixes(clock(hop, piece))
                if hop == 0 and piece == PIECES - 1:
                    lowest_relays()
                    wait_weights(1, 7)
                if hop > 0 and piece == 0:
                    project(-hop)
                if hop > 0 and piece == 1:
                    project(hop)
        project(4)
        prefixes(99.0)
        write_projected()
        received(pieces_of(SPLIT), pair_recv)

        finish_first(1)
        for way in range(2):
            sent(xbuf.at[:6], x_send.at[way])
        sent(xbuf.at[:7], x_pair_send)
        for column in range(COLUMNS):

            @pl.when(x == column)
            def _():
                for condition, prevs in ((z > 0, True), (z == 0, False)):

                    @pl.when(condition)
                    def _():
                        for what, semaphore in (("pair", pair_send), ("right", right_fwd), ("left", left_fwd)):
                            total = count(column, what, prevs)
                            if total:
                                sent(pieces_of(total), semaphore)

                if column < 3:

                    @pl.when(z < LAYERS - 1)
                    def _():
                        sent(pieces_of(2 * SPLIT), relay_send)

    pltpu.make_async_copy(kv_ref.at[8], kv_ref.at[8], local_sem.at[1]).wait()


def gather(slice_rows, w_query, w_key, w_value, prefix_keys, prefix_values):
    bf16, f32 = jnp.bfloat16, jnp.float32
    dma = pltpu.SemaphoreType.DMA
    anywhere = pl.BlockSpec(memory_space=pltpu.HBM)
    vmem = pl.BlockSpec(memory_space=pltpu.VMEM)
    return pl.pallas_call(
        gather_kernel,
        out_shape=(
            pltpu.VMEM((512, HEAD_DIM), bf16),
            pltpu.VMEM((128, HEAD_DIM), bf16),
            pltpu.VMEM((128, HEAD_DIM), bf16),
            pltpu.VMEM((9, 2, 512, HEAD_DIM), bf16),
        ),
        in_specs=[anywhere] * 6,
        out_specs=(vmem,) * 4,
        scratch_shapes=[
            pltpu.VMEM((RING, 128, 512), bf16),
            pltpu.VMEM((RING, 128, 512), bf16),
            pltpu.VMEM((4096, 768), bf16),
            pltpu.VMEM((128, 768), f32),
            pltpu.VMEM((3, 2, 512, HEAD_DIM), bf16),
            dma((2,)), dma((2,)),
            dma((2,)), dma((2, 4 * PIECES)), dma, dma((7,)),
            dma, dma, dma, dma, dma, dma, dma, dma,
            dma((4, SPLIT)), dma((SPLIT,)), dma, pltpu.SemaphoreType.REGULAR,
        ],
        compiler_params=pltpu.CompilerParams(
            collective_id=0, has_side_effects=True, vmem_limit_bytes=58 * 1024 * 1024
        ),
        name="gather",
    )(slice_rows, w_query, w_key, w_value, prefix_keys, prefix_values)


def scores_of(keys, queries):
    return lax.dot_general(
        keys, queries, (((1,), (1,)), ((), ())), preferred_element_type=jnp.float32
    )


def weigh(values, weights):
    return lax.dot_general(
        values, weights, (((0,), (0,)), ((), ())), preferred_element_type=jnp.float32
    )


def attend_kernel(
    blocks_ref, q_ref, k_ref, v_ref, kv_ref, out_ref, scores, m_ref, l_ref, o_ref, pb_ref, out, pb_sem, out_sem
):
    section = lax.axis_index("section")
    factor = math.log2(math.e) / math.sqrt(HEAD_DIM)
    never = 1e30
    live = pltpu.make_async_copy(blocks_ref, pb_ref, pb_sem)
    live.start()
    queries = q_ref[...]

    def slot_of(offset):
        return 8 if offset == 0 else lax.rem(section - offset + 64, 8)

    key_row = lax.broadcasted_iota(jnp.int32, (128, 512), 0)
    query_row = lax.broadcasted_iota(jnp.int32, (128, 512), 1) % 128
    own = jnp.where(key_row <= query_row, scores_of(k_ref[...], queries), -never)
    top = jnp.max(own, axis=0, keepdims=True)
    for offset in range(REACH + 1):
        part = scores_of(kv_ref[slot_of(offset), 0, :BLOCK, :], queries)
        scores[offset] = part
        peak = jnp.max(part, axis=0, keepdims=True)
        top = jnp.maximum(top, jnp.where(section >= offset, peak, -never))
    weights = jnp.exp2((own - top) * factor)
    total = jnp.sum(weights, axis=0, keepdims=True)
    result = weigh(v_ref[...], weights.astype(jnp.bfloat16))
    for offset in range(REACH + 1):
        shift = jnp.where(section >= offset, top, never)
        weights = jnp.exp2((scores[offset] - shift) * factor)
        total += jnp.sum(weights, axis=0, keepdims=True)
        result += weigh(kv_ref[slot_of(offset), 1, :BLOCK, :], weights.astype(jnp.bfloat16))
    m_ref[...] = top
    l_ref[...] = total
    o_ref[...] = result
    live.wait()

    for offset in range(REACH + 1):
        blocks = pb_ref[jnp.maximum(section - offset, 0)]

        @pl.when((section >= offset) & (blocks > 1))
        def _():
            part = scores_of(kv_ref[slot_of(offset), 0, BLOCK:, :], queries)
            before = m_ref[...]
            after = jnp.maximum(before, jnp.max(part, axis=0, keepdims=True))
            keep = jnp.exp2((before - after) * factor)
            weights = jnp.exp2((part - after) * factor)
            m_ref[...] = after
            l_ref[...] = l_ref[...] * keep + jnp.sum(weights, axis=0, keepdims=True)
            o_ref[...] = o_ref[...] * keep + weigh(
                kv_ref[slot_of(offset), 1, BLOCK:, :], weights.astype(jnp.bfloat16)
            )

    final = o_ref[...] / l_ref[...]
    for group in range(4):
        columns = slice(group * 128, (group + 1) * 128)
        out[:, columns] = final[:, columns].T.astype(jnp.bfloat16)
    copy = pltpu.make_async_copy(out, out_ref, out_sem)
    copy.start()
    copy.wait()


def attend(prefix_blocks, queries, own_keys, own_values, kv):
    vmem = pl.BlockSpec(memory_space=pltpu.VMEM)
    return pl.pallas_call(
        attend_kernel,
        out_shape=jax.ShapeDtypeStruct((128, 512), jnp.bfloat16),
        in_specs=[pl.BlockSpec(memory_space=pltpu.HBM)] + [vmem] * 4,
        out_specs=pl.BlockSpec(memory_space=pltpu.HBM),
        scratch_shapes=[
            pltpu.VMEM((REACH + 1, BLOCK, 512), jnp.float32),
            pltpu.VMEM((1, 512), jnp.float32),
            pltpu.VMEM((1, 512), jnp.float32),
            pltpu.VMEM((HEAD_DIM, 512), jnp.float32),
            pltpu.SMEM((64,), jnp.int32),
            pltpu.VMEM((128, 512), jnp.bfloat16),
            pltpu.SemaphoreType.DMA,
            pltpu.SemaphoreType.DMA,
        ],
        compiler_params=pltpu.CompilerParams(vmem_limit_bytes=24 * 1024 * 1024),
        name="attend",
    )(prefix_blocks, queries, own_keys, own_values, kv)


def on_device(slice_rows, w_query, w_key, w_value, prefix_keys, prefix_values, prefix_blocks):
    queries, own_keys, own_values, kv = gather(
        slice_rows, w_query, w_key, w_value, prefix_keys, prefix_values
    )
    return attend(prefix_blocks, queries, own_keys, own_values, kv)


def solution(mesh):
    in_specs = (
        P("section", "head"),
        P(None, "head"),
        P(None, "head"),
        P(None, "head"),
        P("section", "head"),
        P("section", "head"),
        P(),
    )
    out_specs = P("section", "head")
    return jax.shard_map(
        on_device, mesh=mesh, in_specs=in_specs, out_specs=out_specs, check_vma=False
    )
```

```python
import functools
import math

import jax
import jax.numpy as jnp
from jax import lax
from jax.experimental import pallas as pl
from jax.experimental.pallas import tpu as pltpu
from jax.sharding import PartitionSpec as P

HEAD_DIM = 128
BLOCK = 256
REACH = 7
COLUMNS = 4
LAYERS = 8
RING = 8
MESH = pl.DeviceIdType.MESH

SPLIT = 8
ROWS = 2 * 512 // SPLIT
LOW, HIGH = tuple(range(SPLIT // 2)), tuple(range(SPLIT // 2, SPLIT))
LOW_FIRST, HIGH_FIRST = LOW + HIGH, HIGH + LOW
RELAY = 4
PIECES = 8
PIECE = 128 // PIECES


def clock(hop, piece):
    return 3.5 + 2.75 * hop + 2.75 / PIECES * piece


DEFERRED = clock(0, PIECES - 1)


def rows_of(piece):
    return pl.ds((piece // 2) * ROWS, ROWS)


def steps(first, each=5.6 / SPLIT):
    return [first + each * index for index in range(SPLIT)]


def arrivals(column):
    events = []

    def add(times, slot, order=LOW_FIRST, kinds=(0, 1), right=(), left=(), up=(), pair=True, prev=None):
        for time, piece in zip(times, order):
            events.append(
                dict(
                    time=time, slot=slot, kinds=kinds, piece=piece,
                    right=piece in right, left=piece in left, up=piece in up, pair=pair,
                    prev=slot >= column if prev is None else prev,
                )
            )

    every = LOW + HIGH
    direct, relayed = steps(3.5), steps(6.5)
    if column < 3:
        add(steps(7.0, 2.8 / SPLIT), column, kinds=(1,))
        order = HIGH_FIRST if column == 2 else LOW_FIRST
        add(direct, RELAY, order, up=every, pair=False, prev=False)
    if column == 0:
        add(relayed, 1)
        add(steps(7.1), 3, right=LOW)
        add(steps(8.3), 2)
    elif column == 1:
        add(direct, 0, right=LOW)
        add(relayed, 2, left=every)
        add(steps(9.5), 3, LOW)
        add(steps(8.3), 3, HIGH)
    elif column == 2:
        add(direct, 1, right=every)
        add(relayed, 3, HIGH_FIRST, left=HIGH)
        add(steps(8.0), 0, LOW)
        add(steps(8.0), 0, HIGH)
    else:
        add(steps(4.2), 3, right=every)
        add(direct, 2)
        add(direct, 0, HIGH_FIRST, left=HIGH)
        add(steps(8.0), 1)
    return sorted(events, key=lambda event: event["time"])


def gather_kernel(
    x_ref, wq_ref, wk_ref, wv_ref, pk_ref, pv_ref,
    q_ref, k_ref, v_ref, kv_ref,
    xbuf, xother, weights, acc, relay,
    w_sem, local_sem, x_send, x_recv, x_pair_send, x_pair_recv,
    right_send, left_send, up_send, own_send, relay_send, right_fwd, left_fwd, pair_send,
    slot_recv, relay_recv, pair_recv, ready,
):
    section = lax.axis_index("section")
    y = lax.axis_index("head")
    core = lax.rem(section, 2)
    x = lax.rem(lax.div(section, 2), COLUMNS)
    z = lax.div(section, 2 * COLUMNS)

    def at(layer, column, kind, ring=None):
        return ((layer * COLUMNS + column) * 2 + kind, y if ring is None else ring)

    x_right, x_left = lax.rem(x + 1, COLUMNS), lax.rem(x + COLUMNS - 1, COLUMNS)
    z_above, z_below = lax.rem(z + 1, LAYERS), lax.rem(z + LAYERS - 1, LAYERS)
    y_up, y_down = lax.rem(y + 1, RING), lax.rem(y + RING - 1, RING)
    right, left = at(z, x_right, 1), at(z, x_left, 1)
    above = at(z_above, x, 1)
    ways = (at(z, x, 1, y_up), at(z, x, 1, y_down))
    pair = at(z, x, 1 - core)

    def block_at(hop):
        return lax.rem(y + hop + RING, RING)

    visits = [0, -1, 1, -2, 2, -3, 3, 4]

    def start_weights(hop):
        start = pl.multiple_of(block_at(hop) * 512, 512)
        rows = pl.ds(start, 512)
        for source, first, size in ((wq_ref, 0, 512), (wk_ref, 512, 128), (wv_ref, 640, 128)):
            pltpu.make_async_copy(
                source.at[rows], weights.at[rows, first : first + size], w_sem.at[min(abs(hop), 1)]
            ).start()

    def wait_weights(index, blocks):
        rows = weights.at[: blocks * 512]
        pltpu.make_async_copy(rows, rows, w_sem.at[index]).wait()

    def project(hop):
        start = pl.multiple_of(block_at(hop) * 512, 512)
        part = jnp.dot(
            xbuf[block_at(hop)], weights[pl.ds(start, 512), :], preferred_element_type=jnp.float32
        )
        if hop == 0:
            acc[...] = part
        else:
            acc[...] += part

    def write_projected():
        for group in range(4):
            q_ref[group * 128 : (group + 1) * 128, :] = acc[:, group * 128 : (group + 1) * 128].astype(jnp.bfloat16)
        k_ref[...] = acc[:, 512:640].astype(jnp.bfloat16)
        v_ref[...] = acc[:, 640:768].astype(jnp.bfloat16)

    def remote(source, target, send, recv, device):
        return pltpu.make_async_remote_copy(
            src_ref=source, dst_ref=target, send_sem=send, recv_sem=recv,
            device_id=device, device_id_type=MESH,
        )

    own_x = pltpu.make_async_copy(x_ref, xbuf.at[y], local_sem.at[0])

    def tell(semaphore, device):
        pl.semaphore_signal(semaphore, inc=1, device_id=device, device_id_type=MESH)

    barrier = pltpu.get_barrier_semaphore()

    @pl.when(core == 1)
    def _():
        for kind in range(2):
            for device in (
                at(z, x, kind, y_up), at(z, x, kind, y_down),
                at(z, x_right, kind), at(z, x_left, kind),
            ):
                tell(barrier, device)

    tell(barrier, pair)

    @pl.when((z < LAYERS - 1) & ((core == 1) | (x == 3)))
    def _():
        tell(barrier, above)

    own_x.start()
    for hop in visits:
        start_weights(hop)
    pltpu.make_async_copy(pk_ref, kv_ref.at[8, 0], local_sem.at[1]).start()
    pltpu.make_async_copy(pv_ref, kv_ref.at[8, 1], local_sem.at[1]).start()
    below_count = jnp.where((core == 1) & (z > 0), jnp.where(x == 3, 2, 1), 0)
    pl.semaphore_wait(barrier, 5 + below_count)

    @pl.when((core == 1) & (z > 0))
    def _():
        tell(ready, at(z_below, x, 1))

        @pl.when(x == 3)
        def _():
            tell(ready, at(z_below, x, 0))

    def received(here, semaphore):
        remote(here, here, own_send, semaphore, pair).wait_recv()

    def sent(here, semaphore):
        remote(here, here, semaphore, pair_recv, pair).wait_send()

    def pieces_of(count):
        return kv_ref.at[0, 0, : ROWS * count] if count < 3 else kv_ref.at[: count // SPLIT]

    def rows_at(piece):
        return pl.ds(piece * PIECE, PIECE)

    def x_index(hop, piece):
        return hop * PIECES + (piece % (PIECES // 2) if hop == 3 else piece)

    def x_own(way, piece, kind):
        target = xother if kind == 0 else xbuf
        return remote(
            x_ref.at[rows_at(piece)], target.at[y, rows_at(piece)],
            x_send.at[way], x_recv.at[way, piece], ways[way],
        )

    def x_origin(way, hop):
        return block_at(-hop - 1 if way == 0 else hop + 1)

    def x_piece(way, hop, piece, kind):
        return (xother if kind == 0 else xbuf).at[x_origin(way, hop), rows_at(piece)]

    def x_forward(way, hop, piece, kind):
        here = x_piece(way, hop, piece, kind)
        index = x_index(hop + 1, piece)
        return remote(here, here, x_send.at[way], x_recv.at[way, index], ways[way])

    def x_hand(way, hop, piece):
        rows = rows_at(piece)
        return remote(
            xother.at[x_origin(way, hop), rows], xbuf.at[x_origin(way, hop), rows],
            x_pair_send, x_pair_recv.at[min(hop * 2 + way, 6)], pair,
        )

    def travels(way, hop, piece):
        return hop < 3 or (hop == 3 and piece // (PIECES // 2) == way)

    def own_piece(piece):
        return (pk_ref if piece % 2 == 0 else pv_ref).at[rows_of(piece)]

    def slot_piece(column, kind, piece):
        return kv_ref.at[column * 2 + kind, piece % 2, rows_of(piece)]

    def relay_piece(kind, piece):
        return relay.at[kind, piece % 2, rows_of(piece)]

    def send_right(kind, piece, column):
        return remote(
            own_piece(piece), slot_piece(column, kind, piece),
            right_send, slot_recv.at[column, piece], right,
        )

    def send_left(kind, piece, column):
        if column == 0:
            target, arrived = slot_piece(0, kind, piece), slot_recv.at[0, piece]
        else:
            target, arrived = relay_piece(kind, piece), relay_recv.at[piece]
        return remote(own_piece(piece), target, left_send, arrived, left)

    def send_up(kind, piece):
        if kind == 0:
            target, arrived = relay_piece(2, piece), slot_recv.at[x, piece]
        else:
            target, arrived = slot_piece(x, 1, piece), slot_recv.at[x, piece]
        return remote(own_piece(piece), target, up_send, arrived, above)

    def send_pair(piece):
        return remote(
            own_piece(piece), slot_piece(x, 0, piece),
            own_send, pair_recv, pair,
        )

    def first_sends(kind, column):
        leftward = HIGH_FIRST if column in (0, 3) else LOW_FIRST
        for index in range(SPLIT):
            yield column > 0, functools.partial(send_left, kind, leftward[index], column)
            if column < 3:
                yield False, functools.partial(send_right, kind, index, column)

    def source_of(event, column, kind):
        if event["slot"] == RELAY:
            return relay_piece(kind, event["piece"])
        if column == 3 and event["slot"] == 3 and kind == 0:
            return relay_piece(2, event["piece"])
        return slot_piece(event["slot"], kind, event["piece"])

    def sends_of(event, column, upward):
        for kind in event["kinds"]:
            piece, slot = event["piece"], event["slot"]
            source = source_of(event, column, kind)
            if upward:
                if event["up"]:
                    yield remote(
                        source, slot_piece(column + 1, kind, piece), relay_send,
                        slot_recv.at[column + 1, piece], above,
                    )
                continue
            if slot == RELAY:
                continue
            target, arrived = slot_piece(slot, kind, piece), slot_recv.at[slot, piece]
            if event["right"]:
                yield remote(source, target, right_fwd, arrived, right)
            if event["left"]:
                yield remote(source, target, left_fwd, arrived, left)
            if event["pair"] and (slot != column or kind == 1):
                yield remote(source, target, pair_send, pair_recv, pair)

    def count(column, what, prevs):
        total = 0
        for event in arrivals(column):
            if event[what] and (prevs or not event["prev"]):
                kinds = (1,) if what == "pair" and event["slot"] == column else event["kinds"]
                total += len(kinds)
        return total

    def guarded(condition, run):
        if condition is None:
            run()
        else:
            pl.when(condition)(run)

    def start_first(kind):
        for piece in range(PIECES):
            for way in range(2):
                x_own(way, piece, kind).start()
        for column in range(COLUMNS):

            @pl.when(x == column)
            def _():
                plain = [make for needs, make in first_sends(kind, column) if not needs]
                needing = [make for needs, make in first_sends(kind, column) if needs]
                if needing:

                    @pl.when(z < LAYERS - 1)
                    def _():
                        for make in needing:
                            make().start()

                for make in plain:
                    make().start()

    def finish_first(kind):
        @pl.when((x == 0) | (z < LAYERS - 1))
        def _():
            sent(pieces_of(SPLIT), left_send)

        @pl.when(x < 3)
        def _():
            sent(pieces_of(SPLIT), right_send)

        @pl.when((z < LAYERS - 1) & (x == 3) if kind == 0 else z < LAYERS - 1)
        def _():
            sent(pieces_of(SPLIT), up_send)

    @pl.when(z == 0)
    def _():
        for column in range(COLUMNS):

            @pl.when(x == column)
            def _():
                for slot in range(column * 2 + 2, COLUMNS * 2):
                    kv_ref[slot] = jnp.zeros((2, 512, HEAD_DIM), jnp.bfloat16)

                @pl.when(core == 0)
                def _():
                    kv_ref[column * 2 + 1] = jnp.zeros((2, 512, HEAD_DIM), jnp.bfloat16)

    @pl.when(core == 0)
    def _():
        start_first(0)
        for piece in range(SPLIT):
            send_pair(piece).start()
        own_x.wait()
        wait_weights(0, 1)
        project(0)

        @pl.when((x == 3) & (z < LAYERS - 1))
        def _():
            pl.semaphore_wait(ready, 1)
            for piece in range(SPLIT):
                send_up(0, piece).start()

        wait_weights(1, 7)
        for index, hop in enumerate(visits[1:]):
            received(xbuf.at[0], x_pair_recv.at[index])
            project(hop)
        write_projected()

        @pl.when(z > 0)
        def _():
            received(pieces_of(7 * SPLIT), pair_recv)

        for column in range(1, COLUMNS):

            @pl.when((z == 0) & (x == column))
            def _():
                received(pieces_of(2 * SPLIT * column), pair_recv)

        finish_first(0)
        sent(pieces_of(SPLIT), own_send)
        for way in range(2):
            sent(xbuf.at[0], x_send.at[way])

    schedules = [arrivals(column) for column in range(COLUMNS)]

    def handle(event, column):
        def run():
            semaphore = (relay_recv if event["slot"] == RELAY else slot_recv.at[event["slot"]]).at[event["piece"]]
            received(pieces_of(len(event["kinds"])), semaphore)
            if event["up"]:
                held = event["time"] <= DEFERRED

                @pl.when((z > 0) & (z < LAYERS - 1) if held else z < LAYERS - 1)
                def _():
                    for copy in sends_of(event, column, True):
                        copy.start()

            for copy in sends_of(event, column, False):
                copy.start()

        whole = event["slot"] == RELAY and event["up"]
        guarded(z < LAYERS - 1 if whole else z > 0 if event["prev"] else None, run)

    def prefixes(until):
        for column in range(COLUMNS):
            due = [event for event in schedules[column] if event["time"] <= until]
            if not due:
                continue
            schedules[column] = schedules[column][len(due) :]

            @pl.when(x == column)
            def _():
                for event in due:
                    handle(event, column)

    def lowest_goes_up():
        @pl.when(z == 0)
        def _():
            pl.semaphore_wait(ready, 1)
            for piece in range(SPLIT):
                send_up(1, piece).start()

    def lowest_relays():
        for column in range(0, COLUMNS - 1):

            @pl.when((z == 0) & (x == column))
            def _():
                for event in arrivals(column):
                    if event["up"] and event["time"] <= DEFERRED:
                        for copy in sends_of(event, column, True):
                            copy.start()

    @pl.when(core == 1)
    def _():
        start_first(1)

        @pl.when((z > 0) & (z < LAYERS - 1))
        def _():
            pl.semaphore_wait(ready, 1)
            for piece in range(SPLIT):
                send_up(1, piece).start()

        own_x.wait()
        wait_weights(0, 1)
        project(0)
        lowest_goes_up()
        for hop in range(4):
            for piece in range(PIECES):
                if hop == 3 and piece >= PIECES // 2:
                    continue
                for way in range(2):
                    this = piece if hop < 3 or way == 0 else piece + PIECES // 2
                    received(xbuf.at[0, : 2 * PIECE], x_recv.at[way, x_index(hop, this)])
                    for kind in range(2):
                        if travels(way, hop + 1, this):
                            x_forward(way, hop, this, kind).start()
                    x_hand(way, hop, this).start()
                prefixes(clock(hop, piece))
                if hop == 0 and piece == PIECES - 1:
                    lowest_relays()
                    wait_weights(1, 7)
                if hop > 0 and piece == 0:
                    project(-hop)
                if hop > 0 and piece == 1:
                    project(hop)
        project(4)
        prefixes(99.0)
        write_projected()
        received(pieces_of(SPLIT), pair_recv)

        finish_first(1)
        for way in range(2):
            sent(xbuf.at[:6], x_send.at[way])
        sent(xbuf.at[:7], x_pair_send)
        for column in range(COLUMNS):

            @pl.when(x == column)
            def _():
                for condition, prevs in ((z > 0, True), (z == 0, False)):

                    @pl.when(condition)
                    def _():
                        for what, semaphore in (("pair", pair_send), ("right", right_fwd), ("left", left_fwd)):
                            total = count(column, what, prevs)
                            if total:
                                sent(pieces_of(total), semaphore)

                if column < 3:

                    @pl.when(z < LAYERS - 1)
                    def _():
                        sent(pieces_of(2 * SPLIT), relay_send)

    pltpu.make_async_copy(kv_ref.at[8], kv_ref.at[8], local_sem.at[1]).wait()


def gather(slice_rows, w_query, w_key, w_value, prefix_keys, prefix_values):
    bf16, f32 = jnp.bfloat16, jnp.float32
    dma = pltpu.SemaphoreType.DMA
    anywhere = pl.BlockSpec(memory_space=pltpu.HBM)
    vmem = pl.BlockSpec(memory_space=pltpu.VMEM)
    return pl.pallas_call(
        gather_kernel,
        out_shape=(
            pltpu.VMEM((512, HEAD_DIM), bf16),
            pltpu.VMEM((128, HEAD_DIM), bf16),
            pltpu.VMEM((128, HEAD_DIM), bf16),
            pltpu.VMEM((9, 2, 512, HEAD_DIM), bf16),
        ),
        in_specs=[anywhere] * 6,
        out_specs=(vmem,) * 4,
        scratch_shapes=[
            pltpu.VMEM((RING, 128, 512), bf16),
            pltpu.VMEM((RING, 128, 512), bf16),
            pltpu.VMEM((4096, 768), bf16),
            pltpu.VMEM((128, 768), f32),
            pltpu.VMEM((3, 2, 512, HEAD_DIM), bf16),
            dma((2,)), dma((2,)),
            dma((2,)), dma((2, 3 * PIECES + PIECES // 2)), dma, dma((7,)),
            dma, dma, dma, dma, dma, dma, dma, dma,
            dma((4, SPLIT)), dma((SPLIT,)), dma, pltpu.SemaphoreType.REGULAR,
        ],
        compiler_params=pltpu.CompilerParams(
            collective_id=0, has_side_effects=True, vmem_limit_bytes=58 * 1024 * 1024
        ),
        name="gather",
    )(slice_rows, w_query, w_key, w_value, prefix_keys, prefix_values)


def scores_of(keys, queries):
    return lax.dot_general(
        keys, queries, (((1,), (1,)), ((), ())), preferred_element_type=jnp.float32
    )


def weigh(values, weights):
    return lax.dot_general(
        values, weights, (((0,), (0,)), ((), ())), preferred_element_type=jnp.float32
    )


def attend_kernel(
    blocks_ref, q_ref, k_ref, v_ref, kv_ref, out_ref, scores, m_ref, l_ref, o_ref, pb_ref, out, pb_sem, out_sem
):
    section = lax.axis_index("section")
    factor = math.log2(math.e) / math.sqrt(HEAD_DIM)
    never = 1e30
    live = pltpu.make_async_copy(blocks_ref, pb_ref, pb_sem)
    live.start()
    queries = q_ref[...]

    def slot_of(offset):
        return 8 if offset == 0 else lax.rem(section - offset + 64, 8)

    key_row = lax.broadcasted_iota(jnp.int32, (128, 512), 0)
    query_row = lax.broadcasted_iota(jnp.int32, (128, 512), 1) % 128
    own = jnp.where(key_row <= query_row, scores_of(k_ref[...], queries), -never)
    top = jnp.max(own, axis=0, keepdims=True)
    for offset in range(REACH + 1):
        part = scores_of(kv_ref[slot_of(offset), 0, :BLOCK, :], queries)
        scores[offset] = part
        peak = jnp.max(part, axis=0, keepdims=True)
        top = jnp.maximum(top, jnp.where(section >= offset, peak, -never))
    weights = jnp.exp2((own - top) * factor)
    total = jnp.sum(weights, axis=0, keepdims=True)
    result = weigh(v_ref[...], weights.astype(jnp.bfloat16))
    for offset in range(REACH + 1):
        shift = jnp.where(section >= offset, top, never)
        weights = jnp.exp2((scores[offset] - shift) * factor)
        total += jnp.sum(weights, axis=0, keepdims=True)
        result += weigh(kv_ref[slot_of(offset), 1, :BLOCK, :], weights.astype(jnp.bfloat16))
    m_ref[...] = top
    l_ref[...] = total
    o_ref[...] = result
    live.wait()

    for offset in range(REACH + 1):
        blocks = pb_ref[jnp.maximum(section - offset, 0)]

        @pl.when((section >= offset) & (blocks > 1))
        def _():
            part = scores_of(kv_ref[slot_of(offset), 0, BLOCK:, :], queries)
            before = m_ref[...]
            after = jnp.maximum(before, jnp.max(part, axis=0, keepdims=True))
            keep = jnp.exp2((before - after) * factor)
            weights = jnp.exp2((part - after) * factor)
            m_ref[...] = after
            l_ref[...] = l_ref[...] * keep + jnp.sum(weights, axis=0, keepdims=True)
            o_ref[...] = o_ref[...] * keep + weigh(
                kv_ref[slot_of(offset), 1, BLOCK:, :], weights.astype(jnp.bfloat16)
            )

    final = o_ref[...] / l_ref[...]
    for group in range(4):
        columns = slice(group * 128, (group + 1) * 128)
        out[:, columns] = final[:, columns].T.astype(jnp.bfloat16)
    copy = pltpu.make_async_copy(out, out_ref, out_sem)
    copy.start()
    copy.wait()


def attend(prefix_blocks, queries, own_keys, own_values, kv):
    vmem = pl.BlockSpec(memory_space=pltpu.VMEM)
    return pl.pallas_call(
        attend_kernel,
        out_shape=jax.ShapeDtypeStruct((128, 512), jnp.bfloat16),
        in_specs=[pl.BlockSpec(memory_space=pltpu.HBM)] + [vmem] * 4,
        out_specs=pl.BlockSpec(memory_space=pltpu.HBM),
        scratch_shapes=[
            pltpu.VMEM((REACH + 1, BLOCK, 512), jnp.float32),
            pltpu.VMEM((1, 512), jnp.float32),
            pltpu.VMEM((1, 512), jnp.float32),
            pltpu.VMEM((HEAD_DIM, 512), jnp.float32),
            pltpu.SMEM((64,), jnp.int32),
            pltpu.VMEM((128, 512), jnp.bfloat16),
            pltpu.SemaphoreType.DMA,
            pltpu.SemaphoreType.DMA,
        ],
        compiler_params=pltpu.CompilerParams(vmem_limit_bytes=24 * 1024 * 1024),
        name="attend",
    )(prefix_blocks, queries, own_keys, own_values, kv)


def on_device(slice_rows, w_query, w_key, w_value, prefix_keys, prefix_values, prefix_blocks):
    queries, own_keys, own_values, kv = gather(
        slice_rows, w_query, w_key, w_value, prefix_keys, prefix_values
    )
    return attend(prefix_blocks, queries, own_keys, own_values, kv)


def solution(mesh):
    in_specs = (
        P("section", "head"),
        P(None, "head"),
        P(None, "head"),
        P(None, "head"),
        P("section", "head"),
        P("section", "head"),
        P(),
    )
    out_specs = P("section", "head")
    return jax.shard_map(
        on_device, mesh=mesh, in_specs=in_specs, out_specs=out_specs, check_vma=False
    )
```
